32 devices in a mesh: parts: 2 (over y), branch: 2 (over x), seq: 4 (over z), head: 2 (over core).
Axes of the slice: x: 2, y: 2, z: 4, core: 2. Of those that a mesh axis runs over, the one named last changes fastest.
Arguments:
- queries: bfloat16 [4, 48, 8, 128], P(('parts', 'branch'), 'seq', 'head'), parts along dimension 0, may hold values from -160 to 160
- output_cotangent: bfloat16 [4, 48, 8, 128], P(('parts', 'branch'), 'seq', 'head'), parts along dimension 0, may hold values from -6 to 6
- root_keys: bfloat16 [4096, 128], P(('parts', 'seq')), parts along dimension 0, may hold values from -8 to 8
- root_values: bfloat16 [4096, 128], P(('parts', 'seq')), parts along dimension 0, may hold values from -6 to 6
- branch_keys: bfloat16 [4, 2048, 128], P(('parts', 'branch'), 'seq'), parts along dimension 0, may hold values from -6 to 6
- branch_values: bfloat16 [4, 2048, 128], P(('parts', 'branch'), 'seq'), parts along dimension 0, may hold values from -6 to 6
- answer_positions: int32 [4, 48], P(('parts', 'branch')), parts along dimension 0, may hold values from 0 to 2047, as said below
Outputs:
- attention: bfloat16 [4, 48, 8, 128], P(('parts', 'branch'), 'seq', 'head'), parts along dimension 0
- query_gradient: float32 [4, 48, 8, 128], P(('parts', 'branch'), 'seq', 'head'), parts along dimension 0
- root_key_gradient: float32 [4096, 128], P(('parts', 'seq')), parts along dimension 0
- root_value_gradient: float32 [4096, 128], P(('parts', 'seq')), parts along dimension 0
- branch_key_gradient: float32 [4, 2048, 128], P(('parts', 'branch'), 'seq'), parts along dimension 0
- branch_value_gradient: float32 [4, 2048, 128], P(('parts', 'branch'), 'seq'), parts along dimension 0
The draws below stay inside these ranges and needn't reach their ends.
There are 2 independent parts, one for each index of `parts`. The reference program is written for one: setup_inputs(seed, part) draws one part's arguments, and reference() takes and returns one part's arrays. A program takes and returns all parts, laid end to end along the dimension named above; each array names one. Nothing has to cross between parts.
Inputs may be any that keep to these rules, and one draw needn't show every extreme that they name: `answer_positions`: within each branch the positions are strictly increasing.
All inputs are finite; a program needn't handle non-finite values.
Results may differ from the reference program's by a relative error of at most 0.015.
Values may be sent and summed in bfloat16 or wider, within the bound.
No kernel may reach another device: no remote copies, remote signals or barrier semaphores. Data moves between devices by JAX's collectives and lax.ppermute only.
A program may use at most 64 MiB of HBM per device.

```python
import math
import jax
import jax.numpy as jnp
from jax import lax

HD = 128
HEADS = 8
NBR = 2
ROOT = 2048
BLEN = 2048
QA = 48


def shared_keys(key):
    return jax.random.normal(jax.random.fold_in(key, 11), (ROOT, HD), jnp.float32)


def draw_root_keys(key, part):
    return jnp.clip(shared_keys(key), -8.0, 8.0).astype(jnp.bfloat16)


def draw_queries(key, part):
    base = jax.random.normal(jax.random.fold_in(key, 23), (NBR, QA, HEADS, HD), jnp.float32)
    return jnp.clip(base, -160.0, 160.0).astype(jnp.bfloat16)


def draw_answer_positions(key, part):
    drawn = jax.random.randint(jax.random.fold_in(key, 43), (NBR, 1), BLEN // 4, BLEN + 1)
    first_branch = jnp.arange(NBR, dtype=jnp.int32)[:, None] == 0
    lengths = jnp.where(first_branch, BLEN, drawn).astype(jnp.int32)
    index = jnp.arange(QA, dtype=jnp.int32)[None, :]
    spacing = jnp.maximum(lengths // QA, 1)
    start = index * lengths // QA
    jitter = jax.random.randint(jax.random.fold_in(key, 47), (NBR, QA), 0, spacing)
    placed = start + jitter
    placed = jnp.where(index == QA - 1, lengths - 1, placed)
    return placed.astype(jnp.int32)


def block_levels(key, extent, shards, smallest, largest):
    loudness, own = 1.0, jax.random.fold_in(key, 6)
    for axis_at, shards_of in shards:
        heights = jnp.exp(jax.random.uniform(jax.random.fold_in(own, axis_at), (shards_of,), jnp.float32, smallest / len(shards), largest / len(shards)))
        loudness = loudness * jnp.repeat(heights, extent[axis_at] // shards_of).reshape([-1 if axis == axis_at else 1 for axis in range(len(extent))])
    return loudness


def gaussian(key, dims, scale, reach, split=(), kind=jnp.bfloat16):
    result = jax.random.normal(key, dims, jnp.float32) * scale
    if len(split) > 0:
        result = block_levels(key, dims, split, -0.22, 0.18) * result
    return jnp.clip(result, min=-reach, max=reach).astype(kind)


def setup_inputs(seed: int = 0, part: int = 0) -> dict:
    streams_of = jax.random.split(jax.random.key(seed), 8)
    own_keys = jax.random.split(jax.random.fold_in(streams_of[7], part), 8)
    return {
        "queries": draw_queries(jax.random.fold_in(jax.random.fold_in(streams_of[7], part), 71), part),
        "output_cotangent": gaussian(own_keys[1], (NBR, QA, HEADS, HD), 1.0, 6.0, ((0, 2), (1, 4), (2, 2))),
        "root_keys": draw_root_keys(jax.random.fold_in(jax.random.fold_in(streams_of[7], part), 71), part),
        "root_values": gaussian(own_keys[3], (ROOT, HD), 1.0, 6.0, ((0, 4),)),
        "branch_keys": gaussian(own_keys[4], (NBR, BLEN, HD), 1.0, 6.0, ((0, 2), (1, 4))),
        "branch_values": gaussian(own_keys[5], (NBR, BLEN, HD), 1.0, 6.0, ((0, 2), (1, 4))),
        "answer_positions": draw_answer_positions(jax.random.fold_in(jax.random.fold_in(streams_of[7], part), 71), part),
    }


NEG = -1e+30

def reference(queries, output_cotangent, root_keys, root_values, branch_keys, branch_values, answer_positions):
    score_scale = 1.0 / math.sqrt(HD)
    key_index = jnp.arange(ROOT + BLEN, dtype=jnp.int32)

    def one_branch(branch):
        all_keys = jnp.concatenate([root_keys, branch_keys[branch]], 0)
        all_values = jnp.concatenate([root_values, branch_values[branch]], 0)
        places = answer_positions[branch]
        visible = (key_index[None, :] < ROOT) | (key_index[None, :] - ROOT <= places[:, None])

        def one_head(running, head_index):
            query = queries[branch, :, head_index, :]
            cotangent = output_cotangent[branch, :, head_index, :]
            logits = jnp.dot(query, all_keys.T, preferred_element_type=jnp.float32) * score_scale
            logits = jnp.where(visible, logits, NEG)
            peak = lax.optimization_barrier(jnp.max(logits, axis=1))
            probs = jnp.exp(logits - peak[:, None])
            total = lax.optimization_barrier(jnp.sum(probs, axis=1))
            weighted = jnp.dot(probs.astype(jnp.bfloat16), all_values, preferred_element_type=jnp.float32)
            attended_exact = weighted / total[:, None]
            attended = attended_exact.astype(jnp.bfloat16)
            lse = peak + jnp.log(total)
            delta = lax.optimization_barrier(jnp.sum(cotangent.astype(jnp.float32) * attended_exact, axis=1))
            weights = jnp.exp(logits - lse[:, None])
            value_term = jnp.dot(weights.astype(jnp.bfloat16).T, cotangent, preferred_element_type=jnp.float32)
            product = jnp.dot(cotangent, all_values.T, preferred_element_type=jnp.float32)
            slope = (weights * (product - delta[:, None])).astype(jnp.bfloat16)
            query_term = jnp.dot(slope, all_keys, preferred_element_type=jnp.float32) * score_scale
            key_term = jnp.dot(slope.T, query, preferred_element_type=jnp.float32) * score_scale
            return ((running[0] + key_term, running[1] + value_term), (attended, query_term))
        start = (jnp.zeros((ROOT + BLEN, HD), jnp.float32), jnp.zeros((ROOT + BLEN, HD), jnp.float32))
        sums, stacked = lax.scan(one_head, start, jnp.arange(HEADS, dtype=jnp.int32))
        return (stacked[0], stacked[1], sums[0], sums[1])
    attended, query_terms, key_terms, value_terms = lax.map(one_branch, jnp.arange(NBR, dtype=jnp.int32))
    attention = jnp.transpose(attended, (0, 2, 1, 3))
    query_gradient = jnp.transpose(query_terms, (0, 2, 1, 3))
    root_key_gradient = lax.optimization_barrier(jnp.sum(key_terms[:, :ROOT], axis=0))
    root_value_gradient = lax.optimization_barrier(jnp.sum(value_terms[:, :ROOT], axis=0))
    return (attention, query_gradient, root_key_gradient, root_value_gradient, key_terms[:, ROOT:], value_terms[:, ROOT:])
```

```python
import functools
import math

import jax
import jax.numpy as jnp
from jax import lax
from jax.experimental import pallas as pl
from jax.experimental.pallas import tpu as pltpu
from jax.sharding import PartitionSpec as P

NEG = -1e30
LOG2E = math.log2(math.e)
LANES = 128

bf16 = jnp.bfloat16
f32 = jnp.float32


def nt(left, right):
    return lax.dot_general(left, right, (((1,), (1,)), ((), ())), preferred_element_type=f32)


def nn(left, right):
    return jnp.dot(left, right, preferred_element_type=f32)


def cut(total, most):
    if total <= most:
        return [(0, total)]
    size = most
    while total % size or size % LANES:
        size -= LANES
        if size <= 0:
            return [(0, total)]
    return [(at, size) for at in range(0, total, size)]


def lane_tiles(rows):
    tiles = -(-rows // LANES)
    return tiles + tiles % 2


def arrange_kernel(index, gathered, out, *, count, bits, rows):
    place = index[0]
    for target in range(count):
        spot = place ^ target
        at = jnp.int32(0)
        for step, bit in enumerate(bits):
            at = at + (((spot >> bit) & 1) << step)
        start = pl.multiple_of(at * (2 * rows), 16)
        out[0, target * rows:(target + 1) * rows, :] = gathered[pl.ds(start, rows), :]
        start = pl.multiple_of(at * (2 * rows) + rows, 16)
        out[1, target * rows:(target + 1) * rows, :] = gathered[pl.ds(start, rows), :]


def split3(value):
    high = value.astype(bf16).astype(f32)
    rest = value - high
    middle = rest.astype(bf16).astype(f32)
    low = (rest - middle).astype(bf16).astype(f32)
    return high, middle, low


def forward_kernel(index, rows_in, root_k, root_v, branch_k, branch_v, places,
                   own, coded, *rest, count, rows, scale, swap):
    messages, scratch = rest[:-1], rest[-1]
    place = index[0]
    total = count * rows
    tiles = lane_tiles(total)
    branch_count = branch_k.shape[0]
    rk, rv, bk, bv = root_k[...], root_v[...], branch_k[...], branch_v[...]
    stat_columns = []
    for at, size in cut(total, 384):
        query = rows_in[0, at:at + size, :]
        grad = rows_in[1, at:at + size, :]
        root_s = nt(query, rk) * (scale * LOG2E)
        branch_s = nt(query, bk) * (scale * LOG2E)
        key_place = place * branch_count + lax.broadcasted_iota(jnp.int32, (size, branch_count), 1)
        branch_s = jnp.where(key_place <= places[at:at + size, :], branch_s, NEG)
        peak = jnp.maximum(jnp.max(root_s, axis=1, keepdims=True),
                           jnp.max(branch_s, axis=1, keepdims=True))
        root_p = jnp.exp2(root_s - peak)
        branch_p = jnp.exp2(branch_s - peak)
        norm = jnp.sum(root_p, axis=1, keepdims=True) + jnp.sum(branch_p, axis=1, keepdims=True)
        root_d = nt(grad, rv)
        branch_d = nt(grad, bv)
        inverse = 1.0 / norm
        delta = (jnp.sum(root_p * root_d, axis=1, keepdims=True)
                 + jnp.sum(branch_p * branch_d, axis=1, keepdims=True)) * inverse
        root_t = (root_p * (root_d - delta)).astype(bf16)
        branch_t = (branch_p * (branch_d - delta)).astype(bf16)
        root_p = root_p.astype(bf16)
        branch_p = branch_p.astype(bf16)
        scratch[0, at:at + size, :] = (nn(root_p, rv) + nn(branch_p, bv)) * inverse
        scratch[1, at:at + size, :] = (nn(root_t, rk) + nn(branch_t, bk)) * inverse
        scratch[2, at:at + size, :] = (nn(root_p, rk) + nn(branch_p, bk)) * inverse
        lse = peak + jnp.log(norm) * LOG2E
        lane = lax.broadcasted_iota(jnp.int32, (size, LANES), 1)
        packed = jnp.zeros((size, LANES), f32)
        for spot, piece in enumerate(split3(lse) + split3(delta)):
            packed = jnp.where(lane == spot, piece, packed)
        stat_columns.append(packed)
    if tiles * LANES > total:
        stat_columns.append(jnp.zeros((tiles * LANES - total, LANES), f32))
    columns = jnp.concatenate(stat_columns, axis=0)
    stats = [columns[k * LANES:(k + 1) * LANES, :].T[0:8, :] for k in range(tiles)]
    for k in range(tiles):
        coded[:, k * LANES:(k + 1) * LANES] = stats[k]
    stat_rows = jnp.concatenate(stats, axis=0).astype(bf16)

    def piece(which, target):
        start = pl.multiple_of(target * rows, 16)
        return scratch[which, pl.ds(start, rows), :]

    for which in range(3):
        own[which * rows:(which + 1) * rows, :] = piece(which, place)
    if swap:
        for m, message in enumerate(messages):
            for which in range(3):
                message[which * rows:(which + 1) * rows, :] = piece(which, place ^ (m + 1)).astype(bf16)
            message[3 * rows:, :] = stat_rows
    else:
        for target in range(count):
            for which in range(3):
                messages[0][target, which * rows:(which + 1) * rows, :] = piece(which, target).astype(bf16)
            messages[0][target, 3 * rows:, :] = stat_rows


def combine_kernel(coded, *rest, rows, tiles):
    messages, final, every = rest[:-2], rest[-2], rest[-1]
    count = len(messages) + 1
    final[...] = jnp.zeros(final.shape, f32)
    every[...] = jnp.zeros(every.shape, f32)
    for k in range(tiles):
        span = slice(k * LANES, (k + 1) * LANES)
        stats = [coded[:, span]]
        for message in messages:
            both = message[3 * rows + 16 * (k // 2):3 * rows + 16 * (k // 2) + 16, :].astype(f32)
            stats.append(both[8 * (k % 2):8 * (k % 2) + 8, :])
        lses = [s[0:1] + s[1:2] + s[2:3] for s in stats]
        deltas = [s[3:4] + s[4:5] + s[5:6] for s in stats]
        peak = functools.reduce(jnp.maximum, lses)
        shares = [jnp.exp2(v - peak) for v in lses]
        norm = functools.reduce(jnp.add, shares)
        final[0:1, span] = peak + jnp.log(norm) * LOG2E
        final[1:2, span] = functools.reduce(jnp.add, [a * b for a, b in zip(shares, deltas)]) / norm
        for v in range(count):
            every[v:v + 1, span] = lses[v]
            every[count + v:count + v + 1, span] = deltas[v]


def grads_block(keys, values, query, grad, lse, delta, scale, visible=None):
    logits = nt(keys, query) * (scale * LOG2E)
    weights = jnp.exp2(logits - lse)
    if visible is not None:
        weights = jnp.where(visible, weights, 0.0)
    slope = (weights * (nt(values, grad) - delta)).astype(bf16)
    return nn(slope, query), nn(weights.astype(bf16), grad)


def own_branch_kernel(index, mine, other, stats, places, root_k, root_v, branch_k, branch_v,
                      own, every, *rest, count, rows, scale, peers):
    messages = rest[:peers]
    acc_k, acc_v, out_k, out_v, out_a, out_q, query, grad, columns = rest[peers:]
    place, half = index[0], index[1]
    total = count * rows
    heads = 1 if other is None else 2
    start = pl.multiple_of(half * total, 16)
    query[pl.ds(start, total), :] = mine[0]
    grad[pl.ds(start, total), :] = mine[1]
    start = pl.multiple_of((1 - half) * total, 16)
    query[pl.ds(start, total), :] = other[0]
    grad[pl.ds(start, total), :] = other[1]

    def run(keys, values, to_k, to_v, masked):
        size = 256 if keys.shape[0] % 256 == 0 else keys.shape[0]
        for at in range(0, keys.shape[0], size):
            kb, vb = keys[at:at + size, :], values[at:at + size, :]
            sums = None
            for row, width in cut(heads * total, 384):
                visible = None
                if masked:
                    spot = (place * keys.shape[0] + at) + lax.broadcasted_iota(jnp.int32, (size, width), 0)
                    visible = spot <= places[0:1, row:row + width]
                part = grads_block(kb, vb, query[row:row + width, :], grad[row:row + width, :],
                                   stats[0:1, row:row + width], stats[1:2, row:row + width],
                                   scale, visible)
                sums = part if sums is None else (sums[0] + part[0], sums[1] + part[1])
            to_k[at:at + size, :] = sums[0] * scale
            to_v[at:at + size, :] = sums[1]

    run(branch_k, branch_v, out_k, out_v, True)
    run(root_k, root_v, acc_k, acc_v, False)

    tiles = every.shape[1] // LANES
    tall = every.shape[0]
    for k in range(tiles):
        block = every[:, k * LANES:(k + 1) * LANES]
        if tall < LANES:
            block = jnp.concatenate([block, jnp.zeros((LANES - tall, LANES), f32)], axis=0)
        columns[k * LANES:(k + 1) * LANES, :] = block.T
    mine_rows = columns[pl.ds(pl.multiple_of(place * rows, 16), rows), :]
    lses = [mine_rows[:, v:v + 1] for v in range(count)]
    deltas = [mine_rows[:, count + v:count + v + 1] for v in range(count)]
    peak = functools.reduce(jnp.maximum, lses)
    shares = [jnp.exp2(v - peak) for v in lses]
    inverse = 1.0 / functools.reduce(jnp.add, shares)
    shares = [s * inverse for s in shares]
    delta = functools.reduce(jnp.add, [a * b for a, b in zip(shares, deltas)])
    attended = jnp.zeros((rows, LANES), f32)
    slope_sum = jnp.zeros((rows, LANES), f32)
    for v in range(count):
        source = own if v == 0 else messages[v - 1]
        o_part = source[0:rows, :].astype(f32)
        a_part = source[rows:2 * rows, :].astype(f32)
        b_part = source[2 * rows:3 * rows, :].astype(f32)
        attended = attended + shares[v] * o_part
        slope_sum = slope_sum + shares[v] * (a_part + (deltas[v] - delta) * b_part)
    out_a[...] = attended.reshape(out_a.shape).astype(bf16)
    out_q[...] = (slope_sum * scale).reshape(out_q.shape)


def other_branch_kernel(index, acc_k, acc_v, root_k, root_v, *rest, count, rows, scale, others):
    gathered, stats = rest[:others], rest[others:2 * others]
    out_k, out_v, query, grad = rest[2 * others:]
    half = index[1]
    total = count * rows
    for i in range(others):
        start = pl.multiple_of(half * total, 16)
        query[i, pl.ds(start, total), :] = gathered[i][0]
        grad[i, pl.ds(start, total), :] = gathered[i][1]
        start = pl.multiple_of((1 - half) * total, 16)
        query[i, pl.ds(start, total), :] = gathered[i][2]
        grad[i, pl.ds(start, total), :] = gathered[i][3]
    size = 256 if root_k.shape[0] % 256 == 0 else root_k.shape[0]
    for at in range(0, root_k.shape[0], size):
        kb, vb = root_k[at:at + size, :], root_v[at:at + size, :]
        sum_k, sum_v = acc_k[at:at + size, :], acc_v[at:at + size, :]
        for i in range(others):
            sums = None
            for row, width in cut(2 * total, 384):
                part = grads_block(kb, vb, query[i, row:row + width, :], grad[i, row:row + width, :],
                                   stats[i][0:1, row:row + width], stats[i][1:2, row:row + width], scale)
                sums = part if sums is None else (sums[0] + part[0], sums[1] + part[1])
            sum_k = sum_k + sums[0] * scale
            sum_v = sum_v + sums[1]
        out_k[at:at + size, :] = sum_k
        out_v[at:at + size, :] = sum_v


def vmem(n):
    return [pl.BlockSpec(memory_space=pltpu.VMEM)] * n


SMEM = pl.BlockSpec(memory_space=pltpu.SMEM)


def per_device(mesh, queries, output_cotangent, root_keys, root_values,
               branch_keys, branch_values, answer_positions):
    count, branches, heads = mesh.shape["seq"], mesh.shape["branch"], mesh.shape["head"]
    _, answers_here, heads_here, width = queries.shape
    rows = answers_here * heads_here
    total = count * rows
    scale = 1.0 / math.sqrt(width)
    seq_index = lax.axis_index("seq")
    head_index = lax.axis_index("head")
    index = jnp.stack([seq_index, head_index]).astype(jnp.int32)
    root_count = root_keys.shape[0]
    branch_count = branch_keys.shape[1]
    branch_k, branch_v = branch_keys[0], branch_values[0]
    places = jnp.repeat(answer_positions[0], heads_here)
    place_column = places[:, None]
    place_row = jnp.tile(places, heads)[None, :]
    tiles = lane_tiles(total)

    bits = [b for b in reversed(range(count.bit_length() - 1))]
    gathered = jnp.concatenate([queries.reshape(rows, width), output_cotangent.reshape(rows, width)], 0)
    for bit in bits:
        pairs = [(i, i ^ (1 << bit)) for i in range(count)]
        gathered = jnp.concatenate([gathered, lax.ppermute(gathered, "seq", pairs)], 0)
    mine = pl.pallas_call(
        functools.partial(arrange_kernel, count=count, bits=bits, rows=rows),
        out_shape=jax.ShapeDtypeStruct((2, total, width), bf16),
        in_specs=[SMEM] + vmem(1), out_specs=vmem(1)[0], name="arrange",
    )(index, gathered)
    other = lax.ppermute(mine, "head", [(i, (i + 1) % heads) for i in range(heads)])

    swap = count <= 4
    message_rows = 3 * rows + 8 * tiles
    if swap:
        message_shapes = [jax.ShapeDtypeStruct((message_rows, width), bf16)] * (count - 1)
    else:
        message_shapes = [jax.ShapeDtypeStruct((count, message_rows, width), bf16)]
    results = pl.pallas_call(
        functools.partial(forward_kernel, count=count, rows=rows, scale=scale, swap=swap),
        out_shape=[jax.ShapeDtypeStruct((3 * rows, width), f32),
                   jax.ShapeDtypeStruct((8, tiles * LANES), f32)] + message_shapes,
        in_specs=[SMEM] + vmem(6), out_specs=vmem(2 + len(message_shapes)),
        scratch_shapes=[pltpu.VMEM((3, total, width), f32)], name="forward",
    )(index, mine, root_keys, root_values, branch_k, branch_v, place_column)
    own, coded, messages = results[0], results[1], results[2:]
    if swap:
        received = [lax.ppermute(message, "seq", [(i, i ^ (m + 1)) for i in range(count)])
                    for m, message in enumerate(messages)]
    else:
        whole = lax.all_to_all(messages[0], "seq", split_axis=0, concat_axis=0, tiled=True)
        received = [lax.dynamic_index_in_dim(whole, seq_index ^ m, 0, keepdims=False)
                    for m in range(1, count)]

    pair = jnp.concatenate([mine, other], 0)
    pair, messages = lax.optimization_barrier((pair, messages))
    shifts = [[(i, (i + m) % branches) for i in range(branches)] for m in range(1, branches)]
    far = [lax.ppermute(pair, "branch", s) for s in shifts]

    tall = -(-2 * count // 8) * 8
    final, every = pl.pallas_call(
        functools.partial(combine_kernel, rows=rows, tiles=tiles),
        out_shape=[jax.ShapeDtypeStruct((8, tiles * LANES), f32),
                   jax.ShapeDtypeStruct((tall, tiles * LANES), f32)],
        in_specs=vmem(count), out_specs=vmem(2), name="combine",
    )(coded, *received)
    other_final = lax.ppermute(final, "head", [(i, (i + 1) % heads) for i in range(heads)])
    a, b = final[:, :total], other_final[:, :total]
    stats = jnp.where(head_index == 0, jnp.concatenate([a, b], 1), jnp.concatenate([b, a], 1))
    far_stats = [lax.ppermute(stats, "branch", s) for s in shifts]

    acc = jax.ShapeDtypeStruct((root_count, width), f32)
    grad_shape = jax.ShapeDtypeStruct((branch_count, width), f32)
    acc_k, acc_v, branch_gk, branch_gv, attention, query_grad = pl.pallas_call(
        functools.partial(own_branch_kernel, count=count, rows=rows, scale=scale, peers=count - 1),
        out_shape=[acc, acc, grad_shape, grad_shape,
                   jax.ShapeDtypeStruct((answers_here, heads_here, width), bf16),
                   jax.ShapeDtypeStruct((answers_here, heads_here, width), f32)],
        in_specs=[SMEM] + vmem(10 + count - 1), out_specs=vmem(6),
        scratch_shapes=[pltpu.VMEM((heads * total, width), bf16), pltpu.VMEM((heads * total, width), bf16),
                        pltpu.VMEM((tiles * LANES, LANES), f32)], name="own_branch",
    )(index, mine, other, stats, place_row, root_keys, root_values, branch_k, branch_v,
      own, every, *received)
    root_gk, root_gv = pl.pallas_call(
        functools.partial(other_branch_kernel, count=count, rows=rows, scale=scale, others=branches - 1),
        out_shape=[acc, acc],
        in_specs=[SMEM] + vmem(4 + 2 * (branches - 1)), out_specs=vmem(2),
        scratch_shapes=[pltpu.VMEM((branches - 1, heads * total, width), bf16),
                        pltpu.VMEM((branches - 1, heads * total, width), bf16)], name="other_branch",
    )(index, acc_k, acc_v, root_keys, root_values, *far, *far_stats)
    return (attention[None], query_grad[None], root_gk, root_gv, branch_gk[None], branch_gv[None])


def solution(mesh):
    rows = P(("parts", "branch"), "seq", "head", None)
    root = P(("parts", "seq"), None)
    branch = P(("parts", "branch"), "seq", None)
    return jax.shard_map(
        functools.partial(per_device, mesh),
        mesh=mesh,
        in_specs=(rows, rows, root, root, branch, branch, P(("parts", "branch"), None)),
        out_specs=(rows, rows, root, root, branch, branch),
        check_vma=False,
    )
```

```python
import functools
import math

import jax
import jax.numpy as jnp
from jax import lax
from jax.experimental import pallas as pl
from jax.experimental.pallas import tpu as pltpu
from jax.sharding import PartitionSpec as P

NEG = -1e30
LOG2E = math.log2(math.e)
LANES = 128

bf16 = jnp.bfloat16
f32 = jnp.float32


def nt(left, right):
    return lax.dot_general(left, right, (((1,), (1,)), ((), ())), preferred_element_type=f32)


def nn(left, right):
    return jnp.dot(left, right, preferred_element_type=f32)


def cut(total, most):
    if total <= most:
        return [(0, total)]
    size = most
    while total % size or size % LANES:
        size -= LANES
        if size <= 0:
            return [(0, total)]
    return [(at, size) for at in range(0, total, size)]


def lane_tiles(rows):
    tiles = -(-rows // LANES)
    return tiles + tiles % 2


def arrange_kernel(index, gathered, out, *, count, bits, rows):
    place = index[0]
    for target in range(count):
        spot = place ^ target
        at = jnp.int32(0)
        for step, bit in enumerate(bits):
            at = at + (((spot >> bit) & 1) << step)
        start = pl.multiple_of(at * (2 * rows), 16)
        out[0, target * rows:(target + 1) * rows, :] = gathered[pl.ds(start, rows), :]
        start = pl.multiple_of(at * (2 * rows) + rows, 16)
        out[1, target * rows:(target + 1) * rows, :] = gathered[pl.ds(start, rows), :]


def split3(value):
    high = value.astype(bf16).astype(f32)
    rest = value - high
    middle = rest.astype(bf16).astype(f32)
    low = (rest - middle).astype(bf16).astype(f32)
    return high, middle, low


def forward_kernel(index, rows_in, root_k, root_v, branch_k, branch_v, places,
                   own, coded, *rest, count, rows, scale, swap):
    messages, scratch = rest[:-1], rest[-1]
    place = index[0]
    total = count * rows
    tiles = lane_tiles(total)
    branch_count = branch_k.shape[0]
    rk, rv, bk, bv = root_k[...], root_v[...], branch_k[...], branch_v[...]
    stat_columns = []
    for at, size in cut(total, 384):
        query = rows_in[0, at:at + size, :]
        grad = rows_in[1, at:at + size, :]
        root_s = nt(query, rk) * (scale * LOG2E)
        branch_s = nt(query, bk) * (scale * LOG2E)
        key_place = place * branch_count + lax.broadcasted_iota(jnp.int32, (size, branch_count), 1)
        branch_s = jnp.where(key_place <= places[at:at + size, :], branch_s, NEG)
        peak = jnp.maximum(jnp.max(root_s, axis=1, keepdims=True),
                           jnp.max(branch_s, axis=1, keepdims=True))
        root_p = jnp.exp2(root_s - peak)
        branch_p = jnp.exp2(branch_s - peak)
        norm = jnp.sum(root_p, axis=1, keepdims=True) + jnp.sum(branch_p, axis=1, keepdims=True)
        root_d = nt(grad, rv)
        branch_d = nt(grad, bv)
        inverse = 1.0 / norm
        delta = (jnp.sum(root_p * root_d, axis=1, keepdims=True)
                 + jnp.sum(branch_p * branch_d, axis=1, keepdims=True)) * inverse
        root_t = (root_p * (root_d - delta)).astype(bf16)
        branch_t = (branch_p * (branch_d - delta)).astype(bf16)
        root_p = root_p.astype(bf16)
        branch_p = branch_p.astype(bf16)
        scratch[0, at:at + size, :] = (nn(root_p, rv) + nn(branch_p, bv)) * inverse
        scratch[1, at:at + size, :] = (nn(root_t, rk) + nn(branch_t, bk)) * inverse
        scratch[2, at:at + size, :] = (nn(root_p, rk) + nn(branch_p, bk)) * inverse
        lse = peak + jnp.log(norm) * LOG2E
        lane = lax.broadcasted_iota(jnp.int32, (size, LANES), 1)
        packed = jnp.zeros((size, LANES), f32)
        for spot, piece in enumerate(split3(lse) + split3(delta)):
            packed = jnp.where(lane == spot, piece, packed)
        stat_columns.append(packed)
    if tiles * LANES > total:
        stat_columns.append(jnp.zeros((tiles * LANES - total, LANES), f32))
    columns = jnp.concatenate(stat_columns, axis=0)
    stats = [columns[k * LANES:(k + 1) * LANES, :].T[0:8, :] for k in range(tiles)]
    for k in range(tiles):
        coded[:, k * LANES:(k + 1) * LANES] = stats[k]
    stat_rows = jnp.concatenate(stats, axis=0).astype(bf16)

    def piece(which, target):
        start = pl.multiple_of(target * rows, 16)
        return scratch[which, pl.ds(start, rows), :]

    for which in range(3):
        own[which * rows:(which + 1) * rows, :] = piece(which, place)
    if swap:
        for m, message in enumerate(messages):
            for which in range(3):
                message[which * rows:(which + 1) * rows, :] = piece(which, place ^ (m + 1)).astype(bf16)
            message[3 * rows:, :] = stat_rows
    else:
        for target in range(count):
            for which in range(3):
                messages[0][target, which * rows:(which + 1) * rows, :] = piece(which, target).astype(bf16)
            messages[0][target, 3 * rows:, :] = stat_rows


def combine_kernel(coded, *rest, rows, tiles):
    messages, final, every = rest[:-2], rest[-2], rest[-1]
    count = len(messages) + 1
    final[...] = jnp.zeros(final.shape, f32)
    every[...] = jnp.zeros(every.shape, f32)
    for k in range(tiles):
        span = slice(k * LANES, (k + 1) * LANES)
        stats = [coded[:, span]]
        for message in messages:
            both = message[3 * rows + 16 * (k // 2):3 * rows + 16 * (k // 2) + 16, :].astype(f32)
            stats.append(both[8 * (k % 2):8 * (k % 2) + 8, :])
        lses = [s[0:1] + s[1:2] + s[2:3] for s in stats]
        deltas = [s[3:4] + s[4:5] + s[5:6] for s in stats]
        peak = functools.reduce(jnp.maximum, lses)
        shares = [jnp.exp2(v - peak) for v in lses]
        norm = functools.reduce(jnp.add, shares)
        final[0:1, span] = peak + jnp.log(norm) * LOG2E
        final[1:2, span] = functools.reduce(jnp.add, [a * b for a, b in zip(shares, deltas)]) / norm
        for v in range(count):
            every[v:v + 1, span] = lses[v]
            every[count + v:count + v + 1, span] = deltas[v]


def grads_block(keys, values, query, grad, lse, delta, scale, visible=None):
    logits = nt(keys, query) * (scale * LOG2E)
    weights = jnp.exp2(logits - lse)
    if visible is not None:
        weights = jnp.where(visible, weights, 0.0)
    slope = (weights * (nt(values, grad) - delta)).astype(bf16)
    return nn(slope, query), nn(weights.astype(bf16), grad)


def own_branch_kernel(index, mine, other, stats, places, root_k, root_v, branch_k, branch_v,
                      own, every, *rest, count, rows, scale, peers):
    messages = rest[:peers]
    acc_k, acc_v, out_k, out_v, out_a, out_q, query, grad, columns = rest[peers:]
    place, half = index[0], index[1]
    total = count * rows
    heads = 1 if other is None else 2
    start = pl.multiple_of(half * total, 16)
    query[pl.ds(start, total), :] = mine[0]
    grad[pl.ds(start, total), :] = mine[1]
    start = pl.multiple_of((1 - half) * total, 16)
    query[pl.ds(start, total), :] = other[0]
    grad[pl.ds(start, total), :] = other[1]

    def run(keys, values, to_k, to_v, masked):
        size = 256 if keys.shape[0] % 256 == 0 else keys.shape[0]
        for at in range(0, keys.shape[0], size):
            kb, vb = keys[at:at + size, :], values[at:at + size, :]
            sums = None
            for row, width in cut(heads * total, 384):
                visible = None
                if masked:
                    spot = (place * keys.shape[0] + at) + lax.broadcasted_iota(jnp.int32, (size, width), 0)
                    visible = spot <= places[0:1, row:row + width]
                part = grads_block(kb, vb, query[row:row + width, :], grad[row:row + width, :],
                                   stats[0:1, row:row + width], stats[1:2, row:row + width],
                                   scale, visible)
                sums = part if sums is None else (sums[0] + part[0], sums[1] + part[1])
            to_k[at:at + size, :] = sums[0] * scale
            to_v[at:at + size, :] = sums[1]

    run(branch_k, branch_v, out_k, out_v, True)
    run(root_k, root_v, acc_k, acc_v, False)

    tiles = every.shape[1] // LANES
    tall = every.shape[0]
    for k in range(tiles):
        block = every[:, k * LANES:(k + 1) * LANES]
        if tall < LANES:
            block = jnp.concatenate([block, jnp.zeros((LANES - tall, LANES), f32)], axis=0)
        columns[k * LANES:(k + 1) * LANES, :] = block.T
    mine_rows = columns[pl.ds(pl.multiple_of(place * rows, 16), rows), :]
    lses = [mine_rows[:, v:v + 1] for v in range(count)]
    deltas = [mine_rows[:, count + v:count + v + 1] for v in range(count)]
    peak = functools.reduce(jnp.maximum, lses)
    shares = [jnp.exp2(v - peak) for v in lses]
    inverse = 1.0 / functools.reduce(jnp.add, shares)
    shares = [s * inverse for s in shares]
    delta = functools.reduce(jnp.add, [a * b for a, b in zip(shares, deltas)])
    attended = jnp.zeros((rows, LANES), f32)
    slope_sum = jnp.zeros((rows, LANES), f32)
    for v in range(count):
        source = own if v == 0 else messages[v - 1]
        o_part = source[0:rows, :].astype(f32)
        a_part = source[rows:2 * rows, :].astype(f32)
        b_part = source[2 * rows:3 * rows, :].astype(f32)
        attended = attended + shares[v] * o_part
        slope_sum = slope_sum + shares[v] * (a_part + (deltas[v] - delta) * b_part)
    out_a[...] = attended.reshape(out_a.shape).astype(bf16)
    out_q[...] = (slope_sum * scale).reshape(out_q.shape)


def other_branch_kernel(index, acc_k, acc_v, root_k, root_v, *rest, count, rows, scale, others):
    gathered, stats = rest[:others], rest[others:2 * others]
    out_k, out_v, query, grad = rest[2 * others:]
    half = index[1]
    total = count * rows
    for i in range(others):
        start = pl.multiple_of(half * total, 16)
        query[i, pl.ds(start, total), :] = gathered[i][0]
        grad[i, pl.ds(start, total), :] = gathered[i][1]
        start = pl.multiple_of((1 - half) * total, 16)
        query[i, pl.ds(start, total), :] = gathered[i][2]
        grad[i, pl.ds(start, total), :] = gathered[i][3]
    size = 256 if root_k.shape[0] % 256 == 0 else root_k.shape[0]
    for at in range(0, root_k.shape[0], size):
        kb, vb = root_k[at:at + size, :], root_v[at:at + size, :]
        sum_k, sum_v = acc_k[at:at + size, :], acc_v[at:at + size, :]
        for i in range(others):
            sums = None
            for row, width in cut(2 * total, 384):
                part = grads_block(kb, vb, query[i, row:row + width, :], grad[i, row:row + width, :],
                                   stats[i][0:1, row:row + width], stats[i][1:2, row:row + width], scale)
                sums = part if sums is None else (sums[0] + part[0], sums[1] + part[1])
            sum_k = sum_k + sums[0] * scale
            sum_v = sum_v + sums[1]
        out_k[at:at + size, :] = sum_k
        out_v[at:at + size, :] = sum_v


def vmem(n):
    return [pl.BlockSpec(memory_space=pltpu.VMEM)] * n


SMEM = pl.BlockSpec(memory_space=pltpu.SMEM)


def per_device(mesh, queries, output_cotangent, root_keys, root_values,
               branch_keys, branch_values, answer_positions):
    count, branches, heads = mesh.shape["seq"], mesh.shape["branch"], mesh.shape["head"]
    _, answers_here, heads_here, width = queries.shape
    rows = answers_here * heads_here
    total = count * rows
    scale = 1.0 / math.sqrt(width)
    seq_index = lax.axis_index("seq")
    head_index = lax.axis_index("head")
    index = jnp.stack([seq_index, head_index]).astype(jnp.int32)
    root_count = root_keys.shape[0]
    branch_count = branch_keys.shape[1]
    branch_k, branch_v = branch_keys[0], branch_values[0]
    places = jnp.repeat(answer_positions[0], heads_here)
    place_column = places[:, None]
    place_row = jnp.tile(places, heads)[None, :]
    tiles = lane_tiles(total)
    params = pltpu.CompilerParams(vmem_limit_bytes=(20 if total <= 384 else 48) * 2**20)

    bits = [b for b in reversed(range(count.bit_length() - 1))]
    gathered = jnp.concatenate([queries.reshape(rows, width), output_cotangent.reshape(rows, width)], 0)
    for bit in bits:
        pairs = [(i, i ^ (1 << bit)) for i in range(count)]
        gathered = jnp.concatenate([gathered, lax.ppermute(gathered, "seq", pairs)], 0)
    mine = pl.pallas_call(
        functools.partial(arrange_kernel, count=count, bits=bits, rows=rows),
        out_shape=jax.ShapeDtypeStruct((2, total, width), bf16),
        in_specs=[SMEM] + vmem(1), out_specs=vmem(1)[0], name="arrange", compiler_params=params,
    )(index, gathered)
    other = lax.ppermute(mine, "head", [(i, (i + 1) % heads) for i in range(heads)])

    swap = count <= 4
    message_rows = 3 * rows + 8 * tiles
    if swap:
        message_shapes = [jax.ShapeDtypeStruct((message_rows, width), bf16)] * (count - 1)
    else:
        message_shapes = [jax.ShapeDtypeStruct((count, message_rows, width), bf16)]
    results = pl.pallas_call(
        functools.partial(forward_kernel, count=count, rows=rows, scale=scale, swap=swap),
        out_shape=[jax.ShapeDtypeStruct((3 * rows, width), f32),
                   jax.ShapeDtypeStruct((8, tiles * LANES), f32)] + message_shapes,
        in_specs=[SMEM] + vmem(6), out_specs=vmem(2 + len(message_shapes)),
        scratch_shapes=[pltpu.VMEM((3, total, width), f32)], name="forward", compiler_params=params,
    )(index, mine, root_keys, root_values, branch_k, branch_v, place_column)
    own, coded, messages = results[0], results[1], results[2:]
    if swap:
        received = [lax.ppermute(message, "seq", [(i, i ^ (m + 1)) for i in range(count)])
                    for m, message in enumerate(messages)]
    else:
        whole = lax.all_to_all(messages[0], "seq", split_axis=0, concat_axis=0, tiled=True)
        received = [lax.dynamic_index_in_dim(whole, seq_index ^ m, 0, keepdims=False)
                    for m in range(1, count)]

    pair = jnp.concatenate([mine, other], 0)
    pair, messages = lax.optimization_barrier((pair, messages))
    shifts = [[(i, (i + m) % branches) for i in range(branches)] for m in range(1, branches)]
    far = [lax.ppermute(pair, "branch", s) for s in shifts]

    tall = -(-2 * count // 8) * 8
    final, every = pl.pallas_call(
        functools.partial(combine_kernel, rows=rows, tiles=tiles),
        out_shape=[jax.ShapeDtypeStruct((8, tiles * LANES), f32),
                   jax.ShapeDtypeStruct((tall, tiles * LANES), f32)],
        in_specs=vmem(count), out_specs=vmem(2), name="combine", compiler_params=params,
    )(coded, *received)
    other_final = lax.ppermute(final, "head", [(i, (i + 1) % heads) for i in range(heads)])
    a, b = final[:, :total], other_final[:, :total]
    stats = jnp.where(head_index == 0, jnp.concatenate([a, b], 1), jnp.concatenate([b, a], 1))
    far_stats = [lax.ppermute(stats, "branch", s) for s in shifts]

    acc = jax.ShapeDtypeStruct((root_count, width), f32)
    grad_shape = jax.ShapeDtypeStruct((branch_count, width), f32)
    acc_k, acc_v, branch_gk, branch_gv, attention, query_grad = pl.pallas_call(
        functools.partial(own_branch_kernel, count=count, rows=rows, scale=scale, peers=count - 1),
        out_shape=[acc, acc, grad_shape, grad_shape,
                   jax.ShapeDtypeStruct((answers_here, heads_here, width), bf16),
                   jax.ShapeDtypeStruct((answers_here, heads_here, width), f32)],
        in_specs=[SMEM] + vmem(10 + count - 1), out_specs=vmem(6),
        scratch_shapes=[pltpu.VMEM((heads * total, width), bf16), pltpu.VMEM((heads * total, width), bf16),
                        pltpu.VMEM((tiles * LANES, LANES), f32)], name="own_branch", compiler_params=params,
    )(index, mine, other, stats, place_row, root_keys, root_values, branch_k, branch_v,
      own, every, *received)
    root_gk, root_gv = pl.pallas_call(
        functools.partial(other_branch_kernel, count=count, rows=rows, scale=scale, others=branches - 1),
        out_shape=[acc, acc],
        in_specs=[SMEM] + vmem(4 + 2 * (branches - 1)), out_specs=vmem(2),
        scratch_shapes=[pltpu.VMEM((branches - 1, heads * total, width), bf16),
                        pltpu.VMEM((branches - 1, heads * total, width), bf16)], name="other_branch", compiler_params=params,
    )(index, acc_k, acc_v, root_keys, root_values, *far, *far_stats)
    return (attention[None], query_grad[None], root_gk, root_gv, branch_gk[None], branch_gv[None])


def solution(mesh):
    rows = P(("parts", "branch"), "seq", "head", None)
    root = P(("parts", "seq"), None)
    branch = P(("parts", "branch"), "seq", None)
    return jax.shard_map(
        functools.partial(per_device, mesh),
        mesh=mesh,
        in_specs=(rows, rows, root, root, branch, branch, P(("parts", "branch"), None)),
        out_specs=(rows, rows, root, root, branch, branch),
        check_vma=False,
    )
```

```python
import functools
import math

import jax
import jax.numpy as jnp
from jax import lax
from jax.experimental import pallas as pl
from jax.experimental.pallas import tpu as pltpu
from jax.sharding import PartitionSpec as P

NEG = -1e30
LOG2E = math.log2(math.e)
LANES = 128

bf16 = jnp.bfloat16
f32 = jnp.float32


def nt(left, right):
    return lax.dot_general(left, right, (((1,), (1,)), ((), ())), preferred_element_type=f32)


def nn(left, right):
    return jnp.dot(left, right, preferred_element_type=f32)


def total_of(values):
    return functools.reduce(jnp.add, values)


def cut(total, most):
    if total <= most:
        return [(0, total)]
    size = most
    while total % size or size % LANES:
        size -= LANES
        if size <= 0:
            return [(0, total)]
    return [(at, size) for at in range(0, total, size)]


def lane_tiles(rows):
    tiles = -(-rows // LANES)
    return tiles + tiles % 2


def arrange(place, source, base, query, grad, offset, lay):
    for target in range(lay.count):
        spot = place ^ target
        at = jnp.int32(0)
        for step, bit in enumerate(lay.bits):
            at = at + (((spot >> bit) & 1) << step)
        start = pl.multiple_of(base + at * (2 * lay.rows), 16)
        to = pl.multiple_of(offset + target * lay.rows, 16)
        query[pl.ds(to, lay.rows), :] = source[pl.ds(start, lay.rows), :]
        start = pl.multiple_of(base + at * (2 * lay.rows) + lay.rows, 16)
        grad[pl.ds(to, lay.rows), :] = source[pl.ds(start, lay.rows), :]


def split3(value):
    high = value.astype(bf16).astype(f32)
    rest = value - high
    middle = rest.astype(bf16).astype(f32)
    low = (rest - middle).astype(bf16).astype(f32)
    return high, middle, low


def forward_kernel(gathered, root_k, root_v, branch_k, branch_v, places,
                   own, coded, *rest, lay):
    messages, (vectors, query_rows, grad_rows) = rest[:-3], rest[-3:]
    place = lax.axis_index("seq")
    rows, total, tiles = lay.rows, lay.total, lay.tiles
    arrange(place, gathered, 0, query_rows, grad_rows, 0, lay)
    branch_count = branch_k.shape[0]
    rk, rv, bk, bv = root_k[...], root_v[...], branch_k[...], branch_v[...]
    stat_columns = []
    for at, size in cut(total, 384):
        query = query_rows[at:at + size, :]
        grad = grad_rows[at:at + size, :]
        root_s = nt(query, rk) * (lay.scale * LOG2E)
        branch_s = nt(query, bk) * (lay.scale * LOG2E)
        key_place = place * branch_count + lax.broadcasted_iota(jnp.int32, (size, branch_count), 1)
        branch_s = jnp.where(key_place <= places[at:at + size, :], branch_s, NEG)
        peak = jnp.maximum(jnp.max(root_s, axis=1, keepdims=True),
                           jnp.max(branch_s, axis=1, keepdims=True))
        root_p = jnp.exp2(root_s - peak)
        branch_p = jnp.exp2(branch_s - peak)
        norm = jnp.sum(root_p, axis=1, keepdims=True) + jnp.sum(branch_p, axis=1, keepdims=True)
        root_d = nt(grad, rv)
        branch_d = nt(grad, bv)
        inverse = 1.0 / norm
        delta = (jnp.sum(root_p * root_d, axis=1, keepdims=True)
                 + jnp.sum(branch_p * branch_d, axis=1, keepdims=True)) * inverse
        root_t = (root_p * (root_d - delta)).astype(bf16)
        branch_t = (branch_p * (branch_d - delta)).astype(bf16)
        root_p = root_p.astype(bf16)
        branch_p = branch_p.astype(bf16)
        vectors[0, at:at + size, :] = (nn(root_p, rv) + nn(branch_p, bv)) * inverse
        vectors[1, at:at + size, :] = (nn(root_t, rk) + nn(branch_t, bk)) * inverse
        vectors[2, at:at + size, :] = (nn(root_p, rk) + nn(branch_p, bk)) * inverse
        lse = peak + jnp.log(norm) * LOG2E
        lane = lax.broadcasted_iota(jnp.int32, (size, LANES), 1)
        packed = jnp.zeros((size, LANES), f32)
        for spot, piece in enumerate(split3(lse) + split3(delta)):
            packed = jnp.where(lane == spot, piece, packed)
        stat_columns.append(packed)
    if tiles * LANES > total:
        stat_columns.append(jnp.zeros((tiles * LANES - total, LANES), f32))
    columns = jnp.concatenate(stat_columns, axis=0)
    stats = [columns[k * LANES:(k + 1) * LANES, :].T[0:8, :] for k in range(tiles)]
    for k in range(tiles):
        coded[:, k * LANES:(k + 1) * LANES] = stats[k]
    stat_rows = jnp.concatenate(stats, axis=0).astype(bf16)

    def piece(which, target):
        return vectors[which, pl.ds(pl.multiple_of(target * rows, 16), rows), :]

    for which in range(3):
        span = slice(which * rows, (which + 1) * rows)
        own[span, :] = piece(which, place)
        if lay.swap:
            for m, message in enumerate(messages):
                message[span, :] = piece(which, place ^ (m + 1)).astype(bf16)
        else:
            for target in range(lay.count):
                messages[0][target, span, :] = piece(which, target).astype(bf16)
    if lay.swap:
        for message in messages:
            message[3 * rows:, :] = stat_rows
    else:
        for target in range(lay.count):
            messages[0][target, 3 * rows:, :] = stat_rows


def combine_kernel(coded, *rest, lay):
    messages, final, every = rest[:-2], rest[-2], rest[-1]
    rows, count = lay.rows, lay.count
    final[...] = jnp.zeros(final.shape, f32)
    every[...] = jnp.zeros(every.shape, f32)
    for k in range(lay.tiles):
        span = slice(k * LANES, (k + 1) * LANES)
        stats = [coded[:, span]]
        for message in messages:
            both = message[3 * rows + 16 * (k // 2):3 * rows + 16 * (k // 2) + 16, :].astype(f32)
            stats.append(both[8 * (k % 2):8 * (k % 2) + 8, :])
        lses = [s[0:1] + s[1:2] + s[2:3] for s in stats]
        deltas = [s[3:4] + s[4:5] + s[5:6] for s in stats]
        peak = functools.reduce(jnp.maximum, lses)
        shares = [jnp.exp2(v - peak) for v in lses]
        norm = total_of(shares)
        final[0:1, span] = peak + jnp.log(norm) * LOG2E
        final[1:2, span] = total_of([a * b for a, b in zip(shares, deltas)]) / norm
        for v in range(count):
            every[v:v + 1, span] = lses[v]
            every[count + v:count + v + 1, span] = deltas[v]


def local_weights(parts, query, grad, probs, slopes, local, line, logits, products, scale):
    block = 256
    for row, width in cut(query.shape[0], 384):
        lanes = slice(row, row + width)
        q, g = query[lanes, :], grad[lanes, :]
        peak = jnp.full((1, width), NEG, f32)
        spots = []
        for start, keys, values, visible in parts:
            for at in range(0, keys.shape[0], block):
                size = min(block, keys.shape[0] - at)
                s = nt(keys[at:at + size, :], q) * (scale * LOG2E)
                if visible is not None:
                    s = jnp.where(visible(at, size, lanes), s, NEG)
                logits[start + at:start + at + size, 0:width] = s
                products[start + at:start + at + size, 0:width] = nt(values[at:at + size, :], g)
                peak = jnp.maximum(peak, jnp.max(s, axis=0, keepdims=True))
                spots.append(slice(start + at, start + at + size))
        norm = jnp.zeros((1, width), f32)
        weighted = jnp.zeros((1, width), f32)
        for spot in spots:
            p = jnp.exp2(logits[spot, 0:width] - peak)
            logits[spot, 0:width] = p
            probs[spot, lanes] = p.astype(bf16)
            norm = norm + jnp.sum(p, axis=0, keepdims=True)
            weighted = weighted + jnp.sum(p * products[spot, 0:width], axis=0, keepdims=True)
        delta = weighted / norm
        for spot in spots:
            slopes[spot, lanes] = (logits[spot, 0:width] * (products[spot, 0:width] - delta)).astype(bf16)
        local[line:line + 1, lanes] = peak
        local[line + 1:line + 2, lanes] = delta


def own_pre_kernel(mine, other, places, root_k, root_v, branch_k, branch_v,
                   probs, slopes, local, query, grad, logits, products, *, lay):
    place, half = lax.axis_index("seq"), lax.axis_index("head")
    arrange(place, mine, 0, query, grad, half * lay.total, lay)
    arrange(place, other, 0, query, grad, (1 - half) * lay.total, lay)
    count = branch_k.shape[0]

    def visible(at, size, lanes):
        spot = (place * count + at) + lax.broadcasted_iota(jnp.int32, (size, lanes.stop - lanes.start), 0)
        return spot <= places[0:1, lanes]

    local_weights([(0, branch_k, branch_v, visible)], query, grad, probs, slopes, local, 0,
                  logits, products, lay.scale)
    local_weights([(count, root_k, root_v, None)], query, grad, probs, slopes, local, 2,
                  logits, products, lay.scale)


def other_pre_kernel(pair, root_k, root_v, probs, slopes, local, query, grad,
                     logits, products, *, lay):
    place, half = lax.axis_index("seq"), lax.axis_index("head")
    arrange(place, pair, 0, query, grad, half * lay.total, lay)
    arrange(place, pair, 2 * lay.total, query, grad, (1 - half) * lay.total, lay)
    local_weights([(0, root_k, root_v, None)], query, grad, probs, slopes, local, 2,
                  logits, products, lay.scale)


def scaled_rows(local, line, stats, query, grad, both, single, scale):
    for k in range(query.shape[0] // LANES):
        span = slice(k * LANES, (k + 1) * LANES)
        weight = jnp.exp2(local[line:line + 1, span] - stats[0:1, span])
        shift = weight * (local[line + 1:line + 2, span] - stats[1:2, span])
        stacked = jnp.concatenate([weight, shift, jnp.zeros((LANES - 2, LANES), f32)], axis=0)
        columns = stacked.T
        weight, shift = columns[:, 0:1], columns[:, 1:2]
        q = query[span, :].astype(f32) * scale
        both[span, 0:LANES] = (grad[span, :].astype(f32) * weight).astype(bf16)
        both[span, LANES:] = (q * shift).astype(bf16)
        single[span, :] = (q * weight).astype(bf16)


def gradients(probs, slopes, spot, both, single):
    wide = nn(probs[spot, :], both[...])
    return wide[:, LANES:] + nn(slopes[spot, :], single[...]), wide[:, 0:LANES]


def own_final_kernel(probs, slopes, local, query, grad, stats, own, every, *rest, lay):
    messages = rest[:lay.count - 1]
    (acc_k, acc_v, out_a, out_q, out_k, out_v, both, single, columns,
     hold_a, hold_q, hold_k, hold_v, sems) = rest[lay.count - 1:]
    rows, count = lay.rows, lay.count
    copies = []

    def send(source, target, sem):
        copies.append(pltpu.make_async_copy(source, target, sem))
        copies[-1].start()

    tall = every.shape[0]
    for k in range(lay.tiles):
        piece = every[:, k * LANES:(k + 1) * LANES]
        if tall < LANES:
            piece = jnp.concatenate([piece, jnp.zeros((LANES - tall, LANES), f32)], axis=0)
        columns[k * LANES:(k + 1) * LANES, :] = piece.T
    mine_rows = columns[pl.ds(pl.multiple_of(lax.axis_index("seq") * rows, 16), rows), :]
    lses = [mine_rows[:, v:v + 1] for v in range(count)]
    deltas = [mine_rows[:, count + v:count + v + 1] for v in range(count)]
    peak = functools.reduce(jnp.maximum, lses)
    shares = [jnp.exp2(v - peak) for v in lses]
    inverse = 1.0 / total_of(shares)
    shares = [s * inverse for s in shares]
    delta = total_of([a * b for a, b in zip(shares, deltas)])
    attended = jnp.zeros((rows, LANES), f32)
    slope_sum = jnp.zeros((rows, LANES), f32)
    for v in range(count):
        source = own if v == 0 else messages[v - 1]
        o_part = source[0:rows, :].astype(f32)
        a_part = source[rows:2 * rows, :].astype(f32)
        b_part = source[2 * rows:3 * rows, :].astype(f32)
        attended = attended + shares[v] * o_part
        slope_sum = slope_sum + shares[v] * (a_part + (deltas[v] - delta) * b_part)
    hold_a[...] = attended.reshape(out_a.shape).astype(bf16)
    send(hold_a, out_a, sems.at[2, 0])
    hold_q[...] = (slope_sum * lay.scale).reshape(out_q.shape)
    send(hold_q, out_q, sems.at[2, 1])

    branch_count = hold_k.shape[0]
    block = 256
    scaled_rows(local, 0, stats, query, grad, both, single, lay.scale)
    for n, at in enumerate(range(0, branch_count, block)):
        spot = slice(at, min(at + block, branch_count))
        hold_k[spot, :], hold_v[spot, :] = gradients(probs, slopes, spot, both, single)
        send(hold_k.at[spot, :], out_k.at[spot, :], sems.at[0, n])
        send(hold_v.at[spot, :], out_v.at[spot, :], sems.at[1, n])
    scaled_rows(local, 2, stats, query, grad, both, single, lay.scale)
    for at in range(0, acc_k.shape[0], block):
        size = min(block, acc_k.shape[0] - at)
        acc_k[at:at + size, :], acc_v[at:at + size, :] = gradients(
            probs, slopes, slice(branch_count + at, branch_count + at + size), both, single)
    for copy in copies:
        copy.wait()


def other_final_kernel(probs, slopes, local, query, grad, stats, acc_k, acc_v, out_k, out_v,
                       both, single, hold_k, hold_v, sems, *, lay):
    scaled_rows(local, 2, stats, query, grad, both, single, lay.scale)
    count = hold_k.shape[0]
    copies = []
    block = 256
    for n, at in enumerate(range(0, count, block)):
        spot = slice(at, min(at + block, count))
        more_k, more_v = gradients(probs, slopes, spot, both, single)
        hold_k[spot, :] = acc_k[spot, :] + more_k
        copies.append(pltpu.make_async_copy(hold_k.at[spot, :], out_k.at[spot, :], sems.at[0, n]))
        copies[-1].start()
        hold_v[spot, :] = acc_v[spot, :] + more_v
        copies.append(pltpu.make_async_copy(hold_v.at[spot, :], out_v.at[spot, :], sems.at[1, n]))
        copies[-1].start()
    for copy in copies:
        copy.wait()


class Lay:
    def __init__(self, count, rows, scale):
        self.count, self.rows, self.scale = count, rows, scale
        self.total = count * rows
        self.tiles = lane_tiles(self.total)
        self.bits = list(reversed(range(count.bit_length() - 1)))
        self.swap = count <= 4


VMEM = pl.BlockSpec(memory_space=pltpu.VMEM)
ANY = pl.BlockSpec(memory_space=pl.ANY)


def call(kernel, lay, args, outs, scratch=(), away=0):
    specs = [VMEM] * (len(outs) - away) + [ANY] * away
    limit = (20 if lay.total <= 384 else 50) * 2**20
    return pl.pallas_call(
        functools.partial(kernel, lay=lay),
        out_shape=[jax.ShapeDtypeStruct(shape, kind) for shape, kind in outs],
        in_specs=[VMEM] * len(args), out_specs=specs, scratch_shapes=list(scratch),
        compiler_params=pltpu.CompilerParams(vmem_limit_bytes=limit),
    )(*args)


def per_device(mesh, queries, output_cotangent, root_keys, root_values,
               branch_keys, branch_values, answer_positions):
    return body(mesh, queries, output_cotangent, root_keys, root_values,
                branch_keys, branch_values, answer_positions)


def body(mesh, queries, output_cotangent, root_keys, root_values,
         branch_keys, branch_values, answer_positions):
    count, branches, heads = mesh.shape["seq"], mesh.shape["branch"], mesh.shape["head"]
    _, answers_here, heads_here, width = queries.shape
    rows = answers_here * heads_here
    lay = Lay(count, rows, 1.0 / math.sqrt(width))
    total, tiles = lay.total, lay.tiles
    lanes = heads * total
    root_count = root_keys.shape[0]
    branch_count = branch_keys.shape[1]
    branch_k, branch_v = branch_keys[0], branch_values[0]
    seq_index = lax.axis_index("seq")
    head_index = lax.axis_index("head")
    places = jnp.repeat(answer_positions[0], heads_here)
    place_column = places[:, None]
    place_row = jnp.tile(places, heads)[None, :]
    swap_heads = [(i, (i + 1) % heads) for i in range(heads)]
    shifts = [[(i, (i + m) % branches) for i in range(branches)] for m in range(1, branches)]

    gathered = jnp.concatenate([queries.reshape(rows, width), output_cotangent.reshape(rows, width)], 0)
    for bit in lay.bits:
        pairs = [(i, i ^ (1 << bit)) for i in range(count)]
        gathered = jnp.concatenate([gathered, lax.ppermute(gathered, "seq", pairs)], 0)
    other = lax.ppermute(gathered, "head", swap_heads)

    message_rows = 3 * rows + 8 * tiles
    if lay.swap:
        message_shapes = [((message_rows, width), bf16)] * (count - 1)
    else:
        message_shapes = [((count, message_rows, width), bf16)]
    own, coded, *messages = call(
        forward_kernel, lay,
        (gathered, root_keys, root_values, branch_k, branch_v, place_column),
        [((3 * rows, width), f32), ((8, tiles * LANES), f32)] + message_shapes,
        [pltpu.VMEM((3, total, width), f32), pltpu.VMEM((total, width), bf16),
         pltpu.VMEM((total, width), bf16)])
    if lay.swap:
        received = [lax.ppermute(message, "seq", [(i, i ^ (m + 1)) for i in range(count)])
                    for m, message in enumerate(messages)]
    else:
        whole = lax.all_to_all(messages[0], "seq", split_axis=0, concat_axis=0, tiled=True)
        received = [lax.dynamic_index_in_dim(whole, seq_index ^ m, 0, keepdims=False)
                    for m in range(1, count)]

    pair = jnp.concatenate([gathered, other], 0)
    far = [lax.ppermute(pair, "branch", s) for s in shifts]

    def weights_shapes(keys):
        shapes = [((keys, lanes), bf16), ((keys, lanes), bf16), ((8, lanes), f32),
                  ((lanes, width), bf16), ((lanes, width), bf16)]
        wide = cut(lanes, 384)[0][1]
        return shapes, [pltpu.VMEM((keys, wide), f32), pltpu.VMEM((keys, wide), f32)]

    shapes, scratch = weights_shapes(branch_count + root_count)
    own_pre = call(own_pre_kernel, lay,
                   (gathered, other, place_row, root_keys, root_values, branch_k, branch_v),
                   shapes, scratch)

    tall = -(-2 * count // 8) * 8
    final, every = call(combine_kernel, lay, (coded, *received),
                        [((8, tiles * LANES), f32), ((tall, tiles * LANES), f32)])
    other_final = lax.ppermute(final, "head", swap_heads)
    a, b = final[:, :total], other_final[:, :total]
    stats = jnp.where(head_index == 0, jnp.concatenate([a, b], 1), jnp.concatenate([b, a], 1))
    far_stats = [lax.ppermute(stats, "branch", s) for s in shifts]

    def final_scratch(keys):
        blocks = -(-keys // 256)
        return ([pltpu.VMEM((lanes, 2 * width), bf16), pltpu.VMEM((lanes, width), bf16)],
                [pltpu.VMEM((keys, width), f32), pltpu.VMEM((keys, width), f32),
                 pltpu.SemaphoreType.DMA((3, max(2, blocks)))])

    first, last = final_scratch(branch_count)
    sums = ((root_count, width), f32)
    acc_k, acc_v, attention, query_grad, branch_gk, branch_gv = call(
        own_final_kernel, lay, (*own_pre, stats, own, every, *received),
        [sums, sums, ((answers_here, heads_here, width), bf16),
         ((answers_here, heads_here, width), f32),
         ((branch_count, width), f32), ((branch_count, width), f32)],
        first + [pltpu.VMEM((tiles * LANES, LANES), f32),
                 pltpu.VMEM((answers_here, heads_here, width), bf16),
                 pltpu.VMEM((answers_here, heads_here, width), f32)] + last, away=4)
    shapes, scratch = weights_shapes(root_count)
    first, last = final_scratch(root_count)
    for pair, pair_stats in zip(far, far_stats):
        pre = call(other_pre_kernel, lay, (pair, root_keys, root_values),
                   shapes, scratch)
        acc_k, acc_v = call(other_final_kernel, lay, (*pre, pair_stats, acc_k, acc_v),
                            [sums, sums], first + last, away=2)
    return (attention[None], query_grad[None], acc_k, acc_v, branch_gk[None], branch_gv[None])


def solution(mesh):
    rows = P(("parts", "branch"), "seq", "head", None)
    root = P(("parts", "seq"), None)
    branch = P(("parts", "branch"), "seq", None)
    return jax.shard_map(
        functools.partial(per_device, mesh),
        mesh=mesh,
        in_specs=(rows, rows, root, root, branch, branch, P(("parts", "branch"), None)),
        out_specs=(rows, rows, root, root, branch, branch),
        check_vma=False,
    )
```

```python
import functools
import math

import jax
import jax.numpy as jnp
from jax import lax
from jax.experimental import pallas as pl
from jax.experimental.pallas import tpu as pltpu
from jax.sharding import PartitionSpec as P

NEG = -1e30
LOG2E = math.log2(math.e)
LANES = 128
SEQ_FLIPS = (0, 1, 1, 0)
FAR_FLIP = 1
STAT_FLIP = 1

bf16 = jnp.bfloat16
f32 = jnp.float32


def nt(left, right):
    return lax.dot_general(left, right, (((1,), (1,)), ((), ())), preferred_element_type=f32)


def nn(left, right):
    return jnp.dot(left, right, preferred_element_type=f32)


def total_of(values):
    return functools.reduce(jnp.add, values)


def cut(total, most):
    if total <= most:
        return [(0, total)]
    size = most
    while total % size or size % LANES:
        size -= LANES
        if size <= 0:
            return [(0, total)]
    return [(at, size) for at in range(0, total, size)]


def lane_tiles(rows):
    tiles = -(-rows // LANES)
    return tiles + tiles % 2


def arrange(place, source, base, query, grad, offset, lay):
    for target in range(lay.count):
        spot = place ^ target
        at = jnp.int32(0)
        for step, bit in enumerate(lay.bits):
            at = at + (((spot >> bit) & 1) << step)
        start = pl.multiple_of(base + at * (2 * lay.rows), 16)
        to = pl.multiple_of(offset + target * lay.rows, 16)
        query[pl.ds(to, lay.rows), :] = source[pl.ds(start, lay.rows), :]
        start = pl.multiple_of(base + at * (2 * lay.rows) + lay.rows, 16)
        grad[pl.ds(to, lay.rows), :] = source[pl.ds(start, lay.rows), :]


def split3(value):
    high = value.astype(bf16).astype(f32)
    rest = value - high
    middle = rest.astype(bf16).astype(f32)
    low = (rest - middle).astype(bf16).astype(f32)
    return high, middle, low


def forward_kernel(gathered, root_k, root_v, branch_k, branch_v, places,
                   own, coded, *rest, lay):
    messages, (vectors, query_rows, grad_rows) = rest[:-3], rest[-3:]
    place = lax.axis_index("seq")
    rows, total, tiles = lay.rows, lay.total, lay.tiles
    arrange(place, gathered, 0, query_rows, grad_rows, 0, lay)
    branch_count = branch_k.shape[0]
    rk, rv, bk, bv = root_k[...], root_v[...], branch_k[...], branch_v[...]
    stat_columns = []
    for at, size in cut(total, 384):
        query = query_rows[at:at + size, :]
        grad = grad_rows[at:at + size, :]
        root_s = nt(query, rk) * (lay.scale * LOG2E)
        branch_s = nt(query, bk) * (lay.scale * LOG2E)
        key_place = place * branch_count + lax.broadcasted_iota(jnp.int32, (size, branch_count), 1)
        branch_s = jnp.where(key_place <= places[at:at + size, :], branch_s, NEG)
        peak = jnp.maximum(jnp.max(root_s, axis=1, keepdims=True),
                           jnp.max(branch_s, axis=1, keepdims=True))
        root_p = jnp.exp2(root_s - peak)
        branch_p = jnp.exp2(branch_s - peak)
        norm = jnp.sum(root_p, axis=1, keepdims=True) + jnp.sum(branch_p, axis=1, keepdims=True)
        root_d = nt(grad, rv)
        branch_d = nt(grad, bv)
        inverse = 1.0 / norm
        delta = (jnp.sum(root_p * root_d, axis=1, keepdims=True)
                 + jnp.sum(branch_p * branch_d, axis=1, keepdims=True)) * inverse
        root_t = (root_p * (root_d - delta)).astype(bf16)
        branch_t = (branch_p * (branch_d - delta)).astype(bf16)
        root_p = root_p.astype(bf16)
        branch_p = branch_p.astype(bf16)
        vectors[0, at:at + size, :] = (nn(root_p, rv) + nn(branch_p, bv)) * inverse
        vectors[1, at:at + size, :] = (nn(root_t, rk) + nn(branch_t, bk)) * inverse
        vectors[2, at:at + size, :] = (nn(root_p, rk) + nn(branch_p, bk)) * inverse
        lse = peak + jnp.log(norm) * LOG2E
        lane = lax.broadcasted_iota(jnp.int32, (size, LANES), 1)
        packed = jnp.zeros((size, LANES), f32)
        for spot, piece in enumerate(split3(lse) + split3(delta)):
            packed = jnp.where(lane == spot, piece, packed)
        stat_columns.append(packed)
    if tiles * LANES > total:
        stat_columns.append(jnp.zeros((tiles * LANES - total, LANES), f32))
    columns = jnp.concatenate(stat_columns, axis=0)
    stats = [columns[k * LANES:(k + 1) * LANES, :].T[0:8, :] for k in range(tiles)]
    for k in range(tiles):
        coded[:, k * LANES:(k + 1) * LANES] = stats[k]
    stat_rows = jnp.concatenate(stats, axis=0).astype(bf16)

    def piece(which, target):
        return vectors[which, pl.ds(pl.multiple_of(target * rows, 16), rows), :]

    for which in range(3):
        span = slice(which * rows, (which + 1) * rows)
        own[span, :] = piece(which, place)
        if lay.swap:
            for m, message in enumerate(messages):
                message[span, :] = piece(which, place ^ (m + 1)).astype(bf16)
        else:
            for target in range(lay.count):
                messages[0][target, span, :] = piece(which, target).astype(bf16)
    if lay.swap:
        for message in messages:
            message[3 * rows:, :] = stat_rows
    else:
        for target in range(lay.count):
            messages[0][target, 3 * rows:, :] = stat_rows


def combine_kernel(coded, *rest, lay):
    messages, final, every = rest[:-2], rest[-2], rest[-1]
    rows, count = lay.rows, lay.count
    final[...] = jnp.zeros(final.shape, f32)
    every[...] = jnp.zeros(every.shape, f32)
    for k in range(lay.tiles):
        span = slice(k * LANES, (k + 1) * LANES)
        stats = [coded[:, span]]
        for message in messages:
            both = message[3 * rows + 16 * (k // 2):3 * rows + 16 * (k // 2) + 16, :].astype(f32)
            stats.append(both[8 * (k % 2):8 * (k % 2) + 8, :])
        lses = [s[0:1] + s[1:2] + s[2:3] for s in stats]
        deltas = [s[3:4] + s[4:5] + s[5:6] for s in stats]
        peak = functools.reduce(jnp.maximum, lses)
        shares = [jnp.exp2(v - peak) for v in lses]
        norm = total_of(shares)
        final[0:1, span] = peak + jnp.log(norm) * LOG2E
        final[1:2, span] = total_of([a * b for a, b in zip(shares, deltas)]) / norm
        for v in range(count):
            every[v:v + 1, span] = lses[v]
            every[count + v:count + v + 1, span] = deltas[v]


def local_weights(parts, query, grad, probs, slopes, local, line, logits, products, scale):
    block = 256
    for row, width in cut(query.shape[0], 384):
        lanes = slice(row, row + width)
        q, g = query[lanes, :], grad[lanes, :]
        peak = jnp.full((1, width), NEG, f32)
        spots = []
        for start, keys, values, visible in parts:
            for at in range(0, keys.shape[0], block):
                size = min(block, keys.shape[0] - at)
                s = nt(keys[at:at + size, :], q) * (scale * LOG2E)
                if visible is not None:
                    s = jnp.where(visible(at, size, lanes), s, NEG)
                logits[start + at:start + at + size, 0:width] = s
                products[start + at:start + at + size, 0:width] = nt(values[at:at + size, :], g)
                peak = jnp.maximum(peak, jnp.max(s, axis=0, keepdims=True))
                spots.append(slice(start + at, start + at + size))
        norm = jnp.zeros((1, width), f32)
        weighted = jnp.zeros((1, width), f32)
        for spot in spots:
            p = jnp.exp2(logits[spot, 0:width] - peak)
            logits[spot, 0:width] = p
            probs[spot, lanes] = p.astype(bf16)
            norm = norm + jnp.sum(p, axis=0, keepdims=True)
            weighted = weighted + jnp.sum(p * products[spot, 0:width], axis=0, keepdims=True)
        delta = weighted / norm
        for spot in spots:
            slopes[spot, lanes] = (logits[spot, 0:width] * (products[spot, 0:width] - delta)).astype(bf16)
        local[line:line + 1, lanes] = peak
        local[line + 1:line + 2, lanes] = delta


def own_pre_kernel(mine, other, places, root_k, root_v, branch_k, branch_v,
                   probs, slopes, local, query, grad, logits, products, *, lay):
    place, half = lax.axis_index("seq"), lax.axis_index("head")
    arrange(place, mine, 0, query, grad, half * lay.total, lay)
    arrange(place, other, 0, query, grad, (1 - half) * lay.total, lay)
    count = branch_k.shape[0]

    def visible(at, size, lanes):
        spot = (place * count + at) + lax.broadcasted_iota(jnp.int32, (size, lanes.stop - lanes.start), 0)
        return spot <= places[0:1, lanes]

    local_weights([(0, branch_k, branch_v, visible)], query, grad, probs, slopes, local, 0,
                  logits, products, lay.scale)
    local_weights([(count, root_k, root_v, None)], query, grad, probs, slopes, local, 2,
                  logits, products, lay.scale)


def other_pre_kernel(pair, root_k, root_v, probs, slopes, local, query, grad,
                     logits, products, *, lay):
    place, half = lax.axis_index("seq"), lax.axis_index("head") ^ FAR_FLIP
    arrange(place, pair, 0, query, grad, half * lay.total, lay)
    arrange(place, pair, 2 * lay.total, query, grad, (1 - half) * lay.total, lay)
    local_weights([(0, root_k, root_v, None)], query, grad, probs, slopes, local, 2,
                  logits, products, lay.scale)


def scaled_rows(local, line, stats, query, grad, both, single, scale):
    for k in range(query.shape[0] // LANES):
        span = slice(k * LANES, (k + 1) * LANES)
        weight = jnp.exp2(local[line:line + 1, span] - stats[0:1, span])
        shift = weight * (local[line + 1:line + 2, span] - stats[1:2, span])
        stacked = jnp.concatenate([weight, shift, jnp.zeros((LANES - 2, LANES), f32)], axis=0)
        columns = stacked.T
        weight, shift = columns[:, 0:1], columns[:, 1:2]
        q = query[span, :].astype(f32) * scale
        both[span, 0:LANES] = (grad[span, :].astype(f32) * weight).astype(bf16)
        both[span, LANES:] = (q * shift).astype(bf16)
        single[span, :] = (q * weight).astype(bf16)


def gradients(probs, slopes, spot, both, single):
    wide = nn(probs[spot, :], both[...])
    return wide[:, LANES:] + nn(slopes[spot, :], single[...]), wide[:, 0:LANES]


def finish_kernel(own, every, *rest, lay):
    messages, (out_a, out_q, columns) = rest[:-3], rest[-3:]
    rows, count = lay.rows, lay.count
    tall = every.shape[0]
    for k in range(lay.tiles):
        piece = every[:, k * LANES:(k + 1) * LANES]
        if tall < LANES:
            piece = jnp.concatenate([piece, jnp.zeros((LANES - tall, LANES), f32)], axis=0)
        columns[k * LANES:(k + 1) * LANES, :] = piece.T
    mine_rows = columns[pl.ds(pl.multiple_of(lax.axis_index("seq") * rows, 16), rows), :]
    lses = [mine_rows[:, v:v + 1] for v in range(count)]
    deltas = [mine_rows[:, count + v:count + v + 1] for v in range(count)]
    peak = functools.reduce(jnp.maximum, lses)
    shares = [jnp.exp2(v - peak) for v in lses]
    inverse = 1.0 / total_of(shares)
    shares = [s * inverse for s in shares]
    delta = total_of([a * b for a, b in zip(shares, deltas)])
    attended = jnp.zeros((rows, LANES), f32)
    slope_sum = jnp.zeros((rows, LANES), f32)
    for v in range(count):
        source = own if v == 0 else messages[v - 1]
        o_part = source[0:rows, :].astype(f32)
        a_part = source[rows:2 * rows, :].astype(f32)
        b_part = source[2 * rows:3 * rows, :].astype(f32)
        attended = attended + shares[v] * o_part
        slope_sum = slope_sum + shares[v] * (a_part + (deltas[v] - delta) * b_part)
    out_a[...] = attended.reshape(out_a.shape).astype(bf16)
    out_q[...] = (slope_sum * lay.scale).reshape(out_q.shape)


def own_final_kernel(probs, slopes, local, query, grad, stats,
                     acc_k, acc_v, branch_k, branch_v, both, single, *, lay):
    count = branch_k.shape[0]
    block = 256
    for base, line, to_k, to_v in ((0, 0, branch_k, branch_v), (count, 2, acc_k, acc_v)):
        scaled_rows(local, line, stats, query, grad, both, single, lay.scale)
        for at in range(0, to_k.shape[0], block):
            size = min(block, to_k.shape[0] - at)
            to_k[at:at + size, :], to_v[at:at + size, :] = gradients(
                probs, slopes, slice(base + at, base + at + size), both, single)


def other_final_kernel(probs, slopes, local, query, grad, stats, acc_k, acc_v,
                       branch_k, branch_v, attended, query_grad,
                       out_k, out_v, out_bk, out_bv, out_a, out_q,
                       both, single, hold_k, hold_v, sems, *, lay):
    copies = []

    def send(source, target, sem):
        copies.append(pltpu.make_async_copy(source, target, sem))
        copies[-1].start()

    send(branch_k, out_bk, sems.at[2, 0])
    send(branch_v, out_bv, sems.at[2, 1])
    send(attended, out_a, sems.at[3, 0])
    send(query_grad, out_q, sems.at[3, 1])
    scaled_rows(local, 2, stats, query, grad, both, single, lay.scale)
    count = hold_k.shape[0]
    block = 256
    for n, at in enumerate(range(0, count, block)):
        spot = slice(at, min(at + block, count))
        more_k, more_v = gradients(probs, slopes, spot, both, single)
        hold_k[spot, :] = acc_k[spot, :] + more_k
        send(hold_k.at[spot, :], out_k.at[spot, :], sems.at[0, n])
        hold_v[spot, :] = acc_v[spot, :] + more_v
        send(hold_v.at[spot, :], out_v.at[spot, :], sems.at[1, n])
    for copy in copies:
        copy.wait()


class Lay:
    def __init__(self, count, rows, scale):
        self.count, self.rows, self.scale = count, rows, scale
        self.total = count * rows
        self.tiles = lane_tiles(self.total)
        self.bits = list(reversed(range(count.bit_length() - 1)))
        self.swap = count <= 4


VMEM = pl.BlockSpec(memory_space=pltpu.VMEM)
ANY = pl.BlockSpec(memory_space=pl.ANY)


def call(kernel, lay, args, outs, scratch=(), away=0):
    specs = [VMEM] * (len(outs) - away) + [ANY] * away
    limit = (20 if lay.total <= 384 else 50) * 2**20
    return pl.pallas_call(
        functools.partial(kernel, lay=lay),
        out_shape=[jax.ShapeDtypeStruct(shape, kind) for shape, kind in outs],
        in_specs=[VMEM] * len(args), out_specs=specs, scratch_shapes=list(scratch),
        compiler_params=pltpu.CompilerParams(vmem_limit_bytes=limit),
    )(*args)


def move(value, axis, pairs):
    return lax.ppermute(value, axis, pairs)


def per_device(mesh, queries, output_cotangent, root_keys, root_values,
               branch_keys, branch_values, answer_positions):
    return body(mesh, queries, output_cotangent, root_keys, root_values,
                branch_keys, branch_values, answer_positions)


def body(mesh, queries, output_cotangent, root_keys, root_values,
         branch_keys, branch_values, answer_positions):
    count, branches, heads = mesh.shape["seq"], mesh.shape["branch"], mesh.shape["head"]
    _, answers_here, heads_here, width = queries.shape
    rows = answers_here * heads_here
    lay = Lay(count, rows, 1.0 / math.sqrt(width))
    total, tiles = lay.total, lay.tiles
    lanes = heads * total
    root_count = root_keys.shape[0]
    branch_count = branch_keys.shape[1]
    branch_k, branch_v = branch_keys[0], branch_values[0]
    seq_index = lax.axis_index("seq")
    head_index = lax.axis_index("head")
    places = jnp.repeat(answer_positions[0], heads_here)
    place_column = places[:, None]
    place_row = jnp.tile(places, heads)[None, :]
    crossing = lay.swap and heads == 2

    def seq_pairs(m):
        flip = SEQ_FLIPS[m] if crossing else 0
        return [(z * heads + c, (z ^ m) * heads + (c ^ flip)) for z in range(count) for c in range(heads)]

    def far_pairs(m, flip):
        return [(b * heads + c, (b + m) % branches * heads + (c ^ flip))
                for b in range(branches) for c in range(heads)]

    swap_heads = [(i, (i + 1) % heads) for i in range(heads)]
    shifts = range(1, branches)

    gathered = jnp.concatenate([queries.reshape(rows, width), output_cotangent.reshape(rows, width)], 0)
    for bit in lay.bits:
        pairs = seq_pairs(1 << bit)
        gathered = jnp.concatenate([gathered, move(gathered, ("seq", "head"), pairs)], 0)
    other = move(gathered, "head", swap_heads)

    message_rows = 3 * rows + 8 * tiles
    if lay.swap:
        message_shapes = [((message_rows, width), bf16)] * (count - 1)
    else:
        message_shapes = [((count, message_rows, width), bf16)]
    own, coded, *messages = call(
        forward_kernel, lay,
        (gathered, root_keys, root_values, branch_k, branch_v, place_column),
        [((3 * rows, width), f32), ((8, tiles * LANES), f32)] + message_shapes,
        [pltpu.VMEM((3, total, width), f32), pltpu.VMEM((total, width), bf16),
         pltpu.VMEM((total, width), bf16)])
    if lay.swap:
        received = [move(message, ("seq", "head"), seq_pairs(m + 1))
                    for m, message in enumerate(messages)]
    else:
        whole = lax.all_to_all(messages[0], "seq", split_axis=0, concat_axis=0, tiled=True)
        received = [lax.dynamic_index_in_dim(whole, seq_index ^ m, 0, keepdims=False)
                    for m in range(1, count)]

    pair = jnp.concatenate([gathered, other], 0)
    far = [move(pair, ("branch", "head"), far_pairs(m, FAR_FLIP if heads == 2 else 0)) for m in shifts]

    def weights_shapes(keys):
        shapes = [((keys, lanes), bf16), ((keys, lanes), bf16), ((8, lanes), f32),
                  ((lanes, width), bf16), ((lanes, width), bf16)]
        wide = cut(lanes, 384)[0][1]
        return shapes, [pltpu.VMEM((keys, wide), f32), pltpu.VMEM((keys, wide), f32)]

    shapes, scratch = weights_shapes(branch_count + root_count)
    own_pre = call(own_pre_kernel, lay,
                   (gathered, other, place_row, root_keys, root_values, branch_k, branch_v),
                   shapes, scratch)

    tall = -(-2 * count // 8) * 8
    final, every = call(combine_kernel, lay, (coded, *received),
                        [((8, tiles * LANES), f32), ((tall, tiles * LANES), f32)])
    other_final = move(final, "head", swap_heads)
    a, b = final[:, :total], other_final[:, :total]
    stats = jnp.where(head_index == 0, jnp.concatenate([a, b], 1), jnp.concatenate([b, a], 1))
    far_stats = [move(stats, ("branch", "head"), far_pairs(m, STAT_FLIP if heads == 2 else 0)) for m in shifts]

    def final_scratch(keys):
        blocks = -(-keys // 256)
        return ([pltpu.VMEM((lanes, 2 * width), bf16), pltpu.VMEM((lanes, width), bf16)],
                [pltpu.VMEM((keys, width), f32), pltpu.VMEM((keys, width), f32),
                 pltpu.SemaphoreType.DMA((4, max(2, blocks)))])

    row_shapes = [((answers_here, heads_here, width), bf16), ((answers_here, heads_here, width), f32)]
    attention, query_grad = call(
        finish_kernel, lay, (own, every, *received),
        row_shapes, [pltpu.VMEM((tiles * LANES, LANES), f32)])
    root_sum, branch_sum = ((root_count, width), f32), ((branch_count, width), f32)
    first, last = final_scratch(root_count)
    acc_k, acc_v, branch_gk, branch_gv = call(
        own_final_kernel, lay, (*own_pre, stats),
        [root_sum, root_sum, branch_sum, branch_sum], first)
    shapes, scratch = weights_shapes(root_count)
    for pair, pair_stats in zip(far, far_stats):
        pre = call(other_pre_kernel, lay, (pair, root_keys, root_values),
                   shapes, scratch)
        acc_k, acc_v, branch_gk, branch_gv, attention, query_grad = call(
            other_final_kernel, lay,
            (*pre, pair_stats, acc_k, acc_v, branch_gk, branch_gv, attention, query_grad),
            [root_sum, root_sum, branch_sum, branch_sum, *row_shapes], first + last, away=6)
    return (attention[None], query_grad[None], acc_k, acc_v, branch_gk[None], branch_gv[None])


def solution(mesh):
    rows = P(("parts", "branch"), "seq", "head", None)
    root = P(("parts", "seq"), None)
    branch = P(("parts", "branch"), "seq", None)
    return jax.shard_map(
        functools.partial(per_device, mesh),
        mesh=mesh,
        in_specs=(rows, rows, root, root, branch, branch, P(("parts", "branch"), None)),
        out_specs=(rows, rows, root, root, branch, branch),
        check_vma=False,
    )
```

```python
import functools
import math

import jax
import jax.numpy as jnp
from jax import lax
from jax.experimental import pallas as pl
from jax.experimental.pallas import tpu as pltpu
from jax.sharding import PartitionSpec as P

NEG = -1e30
LOG2E = math.log2(math.e)
LANES = 128
SEQ_FLIPS = (0, 1, 1, 0)
FAR_FLIP = 1
STAT_FLIP = 1

bf16 = jnp.bfloat16
f32 = jnp.float32


def nt(left, right):
    return lax.dot_general(left, right, (((1,), (1,)), ((), ())), preferred_element_type=f32)


def nn(left, right):
    return jnp.dot(left, right, preferred_element_type=f32)


def total_of(values):
    return functools.reduce(jnp.add, values)


def cut(total, most):
    if total <= most:
        return [(0, total)]
    size = most
    while total % size or size % LANES:
        size -= LANES
        if size <= 0:
            return [(0, total)]
    return [(at, size) for at in range(0, total, size)]


def lane_tiles(rows):
    tiles = -(-rows // LANES)
    return tiles + tiles % 2


def arrange(place, source, base, query, grad, offset, lay):
    for target in range(lay.count):
        spot = place ^ target
        at = jnp.int32(0)
        for step, bit in enumerate(lay.bits):
            at = at + (((spot >> bit) & 1) << step)
        start = pl.multiple_of(base + at * (2 * lay.rows), 16)
        to = pl.multiple_of(offset + target * lay.rows, 16)
        query[pl.ds(to, lay.rows), :] = source[pl.ds(start, lay.rows), :]
        start = pl.multiple_of(base + at * (2 * lay.rows) + lay.rows, 16)
        grad[pl.ds(to, lay.rows), :] = source[pl.ds(start, lay.rows), :]


def prepare_kernel(root_k, root_v, branch_k, branch_v, positions,
                   to_rk, to_rv, to_bk, to_bv, column, row, hold, sems, *, lay):
    copies = [pltpu.make_async_copy(source, target, sems.at[n]) for n, (source, target) in enumerate(
        [(positions, hold), (root_k, to_rk), (root_v, to_rv), (branch_k, to_bk), (branch_v, to_bv)])]
    for copy in copies:
        copy.start()
    copies[0].wait()
    answers = hold.shape[1]
    known = hold[0:1, :].astype(f32)
    each = lay.total // answers
    for at in range(0, column.shape[0], LANES):
        size = min(LANES, column.shape[0] - at)
        spot = at + lax.broadcasted_iota(jnp.int32, (size, answers), 0)
        spot = jnp.where(spot >= lay.total, spot - lay.total, spot)
        first = each * lax.broadcasted_iota(jnp.int32, (size, answers), 1)
        mine = jnp.where((spot >= first) & (spot < first + each), known, 0.0)
        found = jnp.sum(mine, axis=1, keepdims=True)
        column[at:at + size, :] = found.astype(jnp.int32)
        row[:, at:at + size] = jnp.broadcast_to(found, (size, LANES)).T[0:8, 0:size].astype(jnp.int32)
    for copy in copies[1:]:
        copy.wait()


def split3(value):
    high = value.astype(bf16).astype(f32)
    rest = value - high
    middle = rest.astype(bf16).astype(f32)
    low = (rest - middle).astype(bf16).astype(f32)
    return high, middle, low


def forward_kernel(gathered, root_k, root_v, branch_k, branch_v, places,
                   own, coded, *rest, lay):
    messages, (vectors, query_rows, grad_rows) = rest[:-3], rest[-3:]
    place = lax.axis_index("seq")
    rows, total, tiles = lay.rows, lay.total, lay.tiles
    arrange(place, gathered, 0, query_rows, grad_rows, 0, lay)
    branch_count = branch_k.shape[0]
    rk, rv, bk, bv = root_k[...], root_v[...], branch_k[...], branch_v[...]
    stat_columns = []
    for at, size in cut(total, 384):
        query = query_rows[at:at + size, :]
        grad = grad_rows[at:at + size, :]
        root_s = nt(query, rk) * (lay.scale * LOG2E)
        branch_s = nt(query, bk) * (lay.scale * LOG2E)
        key_place = place * branch_count + lax.broadcasted_iota(jnp.int32, (size, branch_count), 1)
        branch_s = jnp.where(key_place <= places[at:at + size, :], branch_s, NEG)
        peak = jnp.maximum(jnp.max(root_s, axis=1, keepdims=True),
                           jnp.max(branch_s, axis=1, keepdims=True))
        root_p = jnp.exp2(root_s - peak)
        branch_p = jnp.exp2(branch_s - peak)
        norm = jnp.sum(root_p, axis=1, keepdims=True) + jnp.sum(branch_p, axis=1, keepdims=True)
        root_d = nt(grad, rv)
        branch_d = nt(grad, bv)
        inverse = 1.0 / norm
        delta = (jnp.sum(root_p * root_d, axis=1, keepdims=True)
                 + jnp.sum(branch_p * branch_d, axis=1, keepdims=True)) * inverse
        root_t = (root_p * (root_d - delta)).astype(bf16)
        branch_t = (branch_p * (branch_d - delta)).astype(bf16)
        root_p = root_p.astype(bf16)
        branch_p = branch_p.astype(bf16)
        vectors[0, at:at + size, :] = (nn(root_p, rv) + nn(branch_p, bv)) * inverse
        vectors[1, at:at + size, :] = (nn(root_t, rk) + nn(branch_t, bk)) * inverse
        vectors[2, at:at + size, :] = (nn(root_p, rk) + nn(branch_p, bk)) * inverse
        lse = peak + jnp.log(norm) * LOG2E
        lane = lax.broadcasted_iota(jnp.int32, (size, LANES), 1)
        packed = jnp.zeros((size, LANES), f32)
        for spot, piece in enumerate(split3(lse) + split3(delta)):
            packed = jnp.where(lane == spot, piece, packed)
        stat_columns.append(packed)
    if tiles * LANES > total:
        stat_columns.append(jnp.zeros((tiles * LANES - total, LANES), f32))
    columns = jnp.concatenate(stat_columns, axis=0)
    stats = [columns[k * LANES:(k + 1) * LANES, :].T[0:8, :] for k in range(tiles)]
    for k in range(tiles):
        coded[:, k * LANES:(k + 1) * LANES] = stats[k]
    stat_rows = jnp.concatenate(stats, axis=0).astype(bf16)

    def piece(which, target):
        return vectors[which, pl.ds(pl.multiple_of(target * rows, 16), rows), :]

    for which in range(3):
        span = slice(which * rows, (which + 1) * rows)
        own[span, :] = piece(which, place)
        if lay.swap:
            for m, message in enumerate(messages):
                message[span, :] = piece(which, place ^ (m + 1)).astype(bf16)
        else:
            for target in range(lay.count):
                messages[0][target, span, :] = piece(which, target).astype(bf16)
    if lay.swap:
        for message in messages:
            message[3 * rows:, :] = stat_rows
    else:
        for target in range(lay.count):
            messages[0][target, 3 * rows:, :] = stat_rows


def combine_kernel(coded, *rest, lay):
    messages, final, every = rest[:-2], rest[-2], rest[-1]
    rows, count = lay.rows, lay.count
    final[...] = jnp.zeros(final.shape, f32)
    every[...] = jnp.zeros(every.shape, f32)
    for k in range(lay.tiles):
        span = slice(k * LANES, (k + 1) * LANES)
        stats = [coded[:, span]]
        for message in messages:
            both = message[3 * rows + 16 * (k // 2):3 * rows + 16 * (k // 2) + 16, :].astype(f32)
            stats.append(both[8 * (k % 2):8 * (k % 2) + 8, :])
        lses = [s[0:1] + s[1:2] + s[2:3] for s in stats]
        deltas = [s[3:4] + s[4:5] + s[5:6] for s in stats]
        peak = functools.reduce(jnp.maximum, lses)
        shares = [jnp.exp2(v - peak) for v in lses]
        norm = total_of(shares)
        final[0:1, span] = peak + jnp.log(norm) * LOG2E
        final[1:2, span] = total_of([a * b for a, b in zip(shares, deltas)]) / norm
        for v in range(count):
            every[v:v + 1, span] = lses[v]
            every[count + v:count + v + 1, span] = deltas[v]


def local_weights(parts, query, grad, probs, slopes, local, line, logits, products, scale):
    block = 256
    for row, width in cut(query.shape[0], 384):
        lanes = slice(row, row + width)
        q, g = query[lanes, :], grad[lanes, :]
        peak = jnp.full((1, width), NEG, f32)
        spots = []
        for start, keys, values, visible in parts:
            for at in range(0, keys.shape[0], block):
                size = min(block, keys.shape[0] - at)
                s = nt(keys[at:at + size, :], q) * (scale * LOG2E)
                if visible is not None:
                    s = jnp.where(visible(at, size, lanes), s, NEG)
                logits[start + at:start + at + size, 0:width] = s
                products[start + at:start + at + size, 0:width] = nt(values[at:at + size, :], g)
                peak = jnp.maximum(peak, jnp.max(s, axis=0, keepdims=True))
                spots.append(slice(start + at, start + at + size))
        norm = jnp.zeros((1, width), f32)
        weighted = jnp.zeros((1, width), f32)
        for spot in spots:
            p = jnp.exp2(logits[spot, 0:width] - peak)
            logits[spot, 0:width] = p
            probs[spot, lanes] = p.astype(bf16)
            norm = norm + jnp.sum(p, axis=0, keepdims=True)
            weighted = weighted + jnp.sum(p * products[spot, 0:width], axis=0, keepdims=True)
        delta = weighted / norm
        for spot in spots:
            slopes[spot, lanes] = (logits[spot, 0:width] * (products[spot, 0:width] - delta)).astype(bf16)
        local[line:line + 1, lanes] = peak
        local[line + 1:line + 2, lanes] = delta


def own_pre_kernel(mine, other, places, root_k, root_v, branch_k, branch_v,
                   probs, slopes, local, query, grad, logits, products, *, lay):
    place, half = lax.axis_index("seq"), lax.axis_index("head")
    arrange(place, mine, 0, query, grad, half * lay.total, lay)
    arrange(place, other, 0, query, grad, (1 - half) * lay.total, lay)
    count = branch_k.shape[0]

    def visible(at, size, lanes):
        spot = (place * count + at) + lax.broadcasted_iota(jnp.int32, (size, lanes.stop - lanes.start), 0)
        return spot <= places[0:1, lanes]

    local_weights([(0, branch_k, branch_v, visible)], query, grad, probs, slopes, local, 0,
                  logits, products, lay.scale)
    local_weights([(count, root_k, root_v, None)], query, grad, probs, slopes, local, 2,
                  logits, products, lay.scale)


def other_pre_kernel(pair, root_k, root_v, probs, slopes, local, query, grad,
                     logits, products, *, lay):
    place, half = lax.axis_index("seq"), lax.axis_index("head") ^ FAR_FLIP
    arrange(place, pair, 0, query, grad, half * lay.total, lay)
    arrange(place, pair, 2 * lay.total, query, grad, (1 - half) * lay.total, lay)
    local_weights([(0, root_k, root_v, None)], query, grad, probs, slopes, local, 2,
                  logits, products, lay.scale)


def scaled_rows(local, line, stats, query, grad, both, single, scale):
    for k in range(query.shape[0] // LANES):
        span = slice(k * LANES, (k + 1) * LANES)
        weight = jnp.exp2(local[line:line + 1, span] - stats[0:1, span])
        shift = weight * (local[line + 1:line + 2, span] - stats[1:2, span])
        stacked = jnp.concatenate([weight, shift, jnp.zeros((LANES - 2, LANES), f32)], axis=0)
        columns = stacked.T
        weight, shift = columns[:, 0:1], columns[:, 1:2]
        q = query[span, :].astype(f32) * scale
        both[span, 0:LANES] = (grad[span, :].astype(f32) * weight).astype(bf16)
        both[span, LANES:] = (q * shift).astype(bf16)
        single[span, :] = (q * weight).astype(bf16)


def gradients(probs, slopes, spot, both, single):
    wide = nn(probs[spot, :], both[...])
    return wide[:, LANES:] + nn(slopes[spot, :], single[...]), wide[:, 0:LANES]


def finish_kernel(own, every, *rest, lay):
    messages, (out_a, out_q, columns) = rest[:-3], rest[-3:]
    rows, count = lay.rows, lay.count
    tall = every.shape[0]
    for k in range(lay.tiles):
        piece = every[:, k * LANES:(k + 1) * LANES]
        if tall < LANES:
            piece = jnp.concatenate([piece, jnp.zeros((LANES - tall, LANES), f32)], axis=0)
        columns[k * LANES:(k + 1) * LANES, :] = piece.T
    mine_rows = columns[pl.ds(pl.multiple_of(lax.axis_index("seq") * rows, 16), rows), :]
    lses = [mine_rows[:, v:v + 1] for v in range(count)]
    deltas = [mine_rows[:, count + v:count + v + 1] for v in range(count)]
    peak = functools.reduce(jnp.maximum, lses)
    shares = [jnp.exp2(v - peak) for v in lses]
    inverse = 1.0 / total_of(shares)
    shares = [s * inverse for s in shares]
    delta = total_of([a * b for a, b in zip(shares, deltas)])
    attended = jnp.zeros((rows, LANES), f32)
    slope_sum = jnp.zeros((rows, LANES), f32)
    for v in range(count):
        source = own if v == 0 else messages[v - 1]
        o_part = source[0:rows, :].astype(f32)
        a_part = source[rows:2 * rows, :].astype(f32)
        b_part = source[2 * rows:3 * rows, :].astype(f32)
        attended = attended + shares[v] * o_part
        slope_sum = slope_sum + shares[v] * (a_part + (deltas[v] - delta) * b_part)
    out_a[...] = attended.reshape(out_a.shape).astype(bf16)
    out_q[...] = (slope_sum * lay.scale).reshape(out_q.shape)


def own_final_kernel(probs, slopes, local, query, grad, stats,
                     acc_k, acc_v, branch_k, branch_v, both, single, *, lay):
    count = branch_k.shape[0]
    block = 256
    for base, line, to_k, to_v in ((0, 0, branch_k, branch_v), (count, 2, acc_k, acc_v)):
        scaled_rows(local, line, stats, query, grad, both, single, lay.scale)
        for at in range(0, to_k.shape[0], block):
            size = min(block, to_k.shape[0] - at)
            to_k[at:at + size, :], to_v[at:at + size, :] = gradients(
                probs, slopes, slice(base + at, base + at + size), both, single)


def other_final_kernel(probs, slopes, local, query, grad, stats, acc_k, acc_v,
                       branch_k, branch_v, attended, query_grad,
                       out_k, out_v, out_bk, out_bv, out_a, out_q,
                       both, single, hold_k, hold_v, sems, *, lay):
    copies = []

    def send(source, target, sem):
        copies.append(pltpu.make_async_copy(source, target, sem))
        copies[-1].start()

    send(branch_k, out_bk, sems.at[2, 0])
    send(branch_v, out_bv, sems.at[2, 1])
    send(attended, out_a, sems.at[3, 0])
    send(query_grad, out_q, sems.at[3, 1])
    scaled_rows(local, 2, stats, query, grad, both, single, lay.scale)
    count = hold_k.shape[0]
    block = 256
    for n, at in enumerate(range(0, count, block)):
        spot = slice(at, min(at + block, count))
        more_k, more_v = gradients(probs, slopes, spot, both, single)
        hold_k[spot, :] = acc_k[spot, :] + more_k
        send(hold_k.at[spot, :], out_k.at[spot, :], sems.at[0, n])
        hold_v[spot, :] = acc_v[spot, :] + more_v
        send(hold_v.at[spot, :], out_v.at[spot, :], sems.at[1, n])
    for copy in copies:
        copy.wait()


class Lay:
    def __init__(self, count, rows, scale):
        self.count, self.rows, self.scale = count, rows, scale
        self.total = count * rows
        self.tiles = lane_tiles(self.total)
        self.bits = list(range(count.bit_length() - 1))
        self.swap = count <= 4


VMEM = pl.BlockSpec(memory_space=pltpu.VMEM)
ANY = pl.BlockSpec(memory_space=pl.ANY)
HBM = pl.BlockSpec(memory_space=pltpu.HBM)


def call(kernel, lay, args, outs, scratch=(), away=0, far=False):
    specs = [VMEM] * (len(outs) - away) + [ANY] * away
    limit = (20 if lay.total <= 384 else 50) * 2**20
    if far:
        args = [pltpu.with_memory_space_constraint(value, pltpu.HBM) for value in args]
    return pl.pallas_call(
        functools.partial(kernel, lay=lay),
        out_shape=[jax.ShapeDtypeStruct(shape, kind) for shape, kind in outs],
        in_specs=[HBM if far else VMEM] * len(args), out_specs=specs, scratch_shapes=list(scratch),
        compiler_params=pltpu.CompilerParams(vmem_limit_bytes=limit),
    )(*args)


def per_device(mesh, queries, output_cotangent, root_keys, root_values,
               branch_keys, branch_values, answer_positions):
    return body(mesh, queries, output_cotangent, root_keys, root_values,
                branch_keys, branch_values, answer_positions)


def body(mesh, queries, output_cotangent, root_keys, root_values,
         branch_keys, branch_values, answer_positions):
    count, branches, heads = mesh.shape["seq"], mesh.shape["branch"], mesh.shape["head"]
    _, answers_here, heads_here, width = queries.shape
    rows = answers_here * heads_here
    lay = Lay(count, rows, 1.0 / math.sqrt(width))
    total, tiles = lay.total, lay.tiles
    lanes = heads * total
    root_count = root_keys.shape[0]
    branch_count = branch_keys.shape[1]
    seq_index = lax.axis_index("seq")
    head_index = lax.axis_index("head")
    crossing = lay.swap and heads == 2

    def seq_pairs(m):
        flip = SEQ_FLIPS[m] if crossing else 0
        return [(z * heads + c, (z ^ m) * heads + (c ^ flip)) for z in range(count) for c in range(heads)]

    def far_pairs(m, flip):
        return [(b * heads + c, (b + m) % branches * heads + (c ^ flip))
                for b in range(branches) for c in range(heads)]

    swap_heads = [(i, (i + 1) % heads) for i in range(heads)]
    shifts = range(1, branches)

    gathered = jnp.concatenate([queries.reshape(rows, width), output_cotangent.reshape(rows, width)], 0)
    gathered = lax.optimization_barrier(gathered)
    if lay.swap:
        gathered = jnp.concatenate([gathered] + [
            lax.ppermute(gathered, ("seq", "head"), seq_pairs(m)) for m in range(1, count)], 0)
    else:
        for bit in lay.bits:
            pairs = seq_pairs(1 << bit)
            gathered = jnp.concatenate([gathered, lax.ppermute(gathered, ("seq", "head"), pairs)], 0)
    keys = [((root_count, width), bf16)] * 2 + [((branch_count, width), bf16)] * 2
    root_k, root_v, branch_k, branch_v, place_column, place_row = call(
        prepare_kernel, lay, (root_keys, root_values, branch_keys[0], branch_values[0], answer_positions),
        keys + [((lanes, 1), jnp.int32), ((8, lanes), jnp.int32)],
        [pltpu.VMEM(answer_positions.shape, jnp.int32), pltpu.SemaphoreType.DMA((5,))], far=True)
    other = lax.ppermute(gathered, "head", swap_heads)

    message_rows = 3 * rows + 8 * tiles
    if lay.swap:
        message_shapes = [((message_rows, width), bf16)] * (count - 1)
    else:
        message_shapes = [((count, message_rows, width), bf16)]
    own, coded, *messages = call(
        forward_kernel, lay,
        (gathered, root_k, root_v, branch_k, branch_v, place_column),
        [((3 * rows, width), f32), ((8, tiles * LANES), f32)] + message_shapes,
        [pltpu.VMEM((3, total, width), f32), pltpu.VMEM((total, width), bf16),
         pltpu.VMEM((total, width), bf16)])
    if lay.swap:
        received = [lax.ppermute(message, ("seq", "head"), seq_pairs(m + 1))
                    for m, message in enumerate(messages)]
    else:
        whole = lax.all_to_all(messages[0], "seq", split_axis=0, concat_axis=0, tiled=True)
        received = [lax.dynamic_index_in_dim(whole, seq_index ^ m, 0, keepdims=False)
                    for m in range(1, count)]

    pair = jnp.concatenate([gathered, other], 0)
    far = [lax.ppermute(pair, ("branch", "head"), far_pairs(m, FAR_FLIP if heads == 2 else 0)) for m in shifts]

    def weights_shapes(keys):
        shapes = [((keys, lanes), bf16), ((keys, lanes), bf16), ((8, lanes), f32),
                  ((lanes, width), bf16), ((lanes, width), bf16)]
        wide = cut(lanes, 384)[0][1]
        return shapes, [pltpu.VMEM((keys, wide), f32), pltpu.VMEM((keys, wide), f32)]

    shapes, scratch = weights_shapes(branch_count + root_count)
    own_pre = call(own_pre_kernel, lay,
                   (gathered, other, place_row, root_k, root_v, branch_k, branch_v),
                   shapes, scratch)

    tall = -(-2 * count // 8) * 8
    final, every = call(combine_kernel, lay, (coded, *received),
                        [((8, tiles * LANES), f32), ((tall, tiles * LANES), f32)])
    other_final = lax.ppermute(final, "head", swap_heads)
    a, b = final[:, :total], other_final[:, :total]
    stats = jnp.where(head_index == 0, jnp.concatenate([a, b], 1), jnp.concatenate([b, a], 1))
    far_stats = [lax.ppermute(stats, ("branch", "head"), far_pairs(m, STAT_FLIP if heads == 2 else 0)) for m in shifts]

    def final_scratch(keys):
        blocks = -(-keys // 256)
        return ([pltpu.VMEM((lanes, 2 * width), bf16), pltpu.VMEM((lanes, width), bf16)],
                [pltpu.VMEM((keys, width), f32), pltpu.VMEM((keys, width), f32),
                 pltpu.SemaphoreType.DMA((4, max(2, blocks)))])

    row_shapes = [((answers_here, heads_here, width), bf16), ((answers_here, heads_here, width), f32)]
    attention, query_grad = call(
        finish_kernel, lay, (own, every, *received),
        row_shapes, [pltpu.VMEM((tiles * LANES, LANES), f32)])
    root_sum, branch_sum = ((root_count, width), f32), ((branch_count, width), f32)
    first, last = final_scratch(root_count)
    acc_k, acc_v, branch_gk, branch_gv = call(
        own_final_kernel, lay, (*own_pre, stats),
        [root_sum, root_sum, branch_sum, branch_sum], first)
    shapes, scratch = weights_shapes(root_count)
    for pair, pair_stats in zip(far, far_stats):
        pre = call(other_pre_kernel, lay, (pair, root_k, root_v),
                   shapes, scratch)
        acc_k, acc_v, branch_gk, branch_gv, attention, query_grad = call(
            other_final_kernel, lay,
            (*pre, pair_stats, acc_k, acc_v, branch_gk, branch_gv, attention, query_grad),
            [root_sum, root_sum, branch_sum, branch_sum, *row_shapes], first + last, away=6)
    return (attention[None], query_grad[None], acc_k, acc_v, branch_gk[None], branch_gv[None])


def solution(mesh):
    rows = P(("parts", "branch"), "seq", "head", None)
    root = P(("parts", "seq"), None)
    branch = P(("parts", "branch"), "seq", None)
    return jax.shard_map(
        functools.partial(per_device, mesh),
        mesh=mesh,
        in_specs=(rows, rows, root, root, branch, branch, P(("parts", "branch"), None)),
        out_specs=(rows, rows, root, root, branch, branch),
        check_vma=False,
    )
```

```python
import functools
import math

import jax
import jax.numpy as jnp
from jax import lax
from jax.experimental import pallas as pl
from jax.experimental.pallas import tpu as pltpu
from jax.sharding import PartitionSpec as P

NEG = -1e30
LOG2E = math.log2(math.e)
LANES = 128
SEQ_FLIPS = (0, 1, 1, 0)
FAR_FLIP = 1
STAT_FLIP = 1

bf16 = jnp.bfloat16
f32 = jnp.float32


def nt(left, right):
    return lax.dot_general(left, right, (((1,), (1,)), ((), ())), preferred_element_type=f32)


def nn(left, right):
    return jnp.dot(left, right, preferred_element_type=f32)


def total_of(values):
    return functools.reduce(jnp.add, values)


def cut(total, most):
    if total <= most:
        return [(0, total)]
    size = most
    while total % size or size % LANES:
        size -= LANES
        if size <= 0:
            return [(0, total)]
    return [(at, size) for at in range(0, total, size)]


def lane_tiles(rows):
    tiles = -(-rows // LANES)
    return tiles + tiles % 2


def arrange(place, source, base, query, grad, offset, lay):
    for target in range(lay.count):
        spot = place ^ target
        at = jnp.int32(0)
        for step, bit in enumerate(lay.bits):
            at = at + (((spot >> bit) & 1) << step)
        start = pl.multiple_of(base + at * (2 * lay.rows), 16)
        to = pl.multiple_of(offset + target * lay.rows, 16)
        query[pl.ds(to, lay.rows), :] = source[pl.ds(start, lay.rows), :]
        start = pl.multiple_of(base + at * (2 * lay.rows) + lay.rows, 16)
        grad[pl.ds(to, lay.rows), :] = source[pl.ds(start, lay.rows), :]


def prepare_kernel(root_k, root_v, branch_k, branch_v, positions,
                   to_rk, to_rv, to_bk, to_bv, column, row, hold, sems, *, lay):
    copies = [pltpu.make_async_copy(source, target, sems.at[n]) for n, (source, target) in enumerate(
        [(positions, hold), (root_k, to_rk), (root_v, to_rv), (branch_k, to_bk), (branch_v, to_bv)])]
    for copy in copies:
        copy.start()
    copies[0].wait()
    answers = hold.shape[1]
    known = hold[0:1, :].astype(f32)
    each = lay.total // answers
    for at in range(0, column.shape[0], LANES):
        size = min(LANES, column.shape[0] - at)
        spot = at + lax.broadcasted_iota(jnp.int32, (size, answers), 0)
        spot = jnp.where(spot >= lay.total, spot - lay.total, spot)
        first = each * lax.broadcasted_iota(jnp.int32, (size, answers), 1)
        mine = jnp.where((spot >= first) & (spot < first + each), known, 0.0)
        found = jnp.sum(mine, axis=1, keepdims=True)
        column[at:at + size, :] = found.astype(jnp.int32)
        row[:, at:at + size] = jnp.broadcast_to(found, (size, LANES)).T[0:8, 0:size].astype(jnp.int32)
    for copy in copies[1:]:
        copy.wait()


def split3(value):
    high = value.astype(bf16).astype(f32)
    rest = value - high
    middle = rest.astype(bf16).astype(f32)
    low = (rest - middle).astype(bf16).astype(f32)
    return high, middle, low


def attend(query, grad, places, keys, place, scale):
    rk, rv, bk, bv = keys
    size, branch_count = query.shape[0], bk.shape[0]
    root_s = nt(query, rk) * (scale * LOG2E)
    branch_s = nt(query, bk) * (scale * LOG2E)
    key_place = place * branch_count + lax.broadcasted_iota(jnp.int32, (size, branch_count), 1)
    branch_s = jnp.where(key_place <= places, branch_s, NEG)
    peak = jnp.maximum(jnp.max(root_s, axis=1, keepdims=True),
                       jnp.max(branch_s, axis=1, keepdims=True))
    root_p = jnp.exp2(root_s - peak)
    branch_p = jnp.exp2(branch_s - peak)
    norm = jnp.sum(root_p, axis=1, keepdims=True) + jnp.sum(branch_p, axis=1, keepdims=True)
    root_d = nt(grad, rv)
    branch_d = nt(grad, bv)
    inverse = 1.0 / norm
    delta = (jnp.sum(root_p * root_d, axis=1, keepdims=True)
             + jnp.sum(branch_p * branch_d, axis=1, keepdims=True)) * inverse
    root_t = (root_p * (root_d - delta)).astype(bf16)
    branch_t = (branch_p * (branch_d - delta)).astype(bf16)
    root_p = root_p.astype(bf16)
    branch_p = branch_p.astype(bf16)
    vectors = ((nn(root_p, rv) + nn(branch_p, bv)) * inverse,
               (nn(root_t, rk) + nn(branch_t, bk)) * inverse,
               (nn(root_p, rk) + nn(branch_p, bk)) * inverse)
    lse = peak + jnp.log(norm) * LOG2E
    lane = lax.broadcasted_iota(jnp.int32, (size, LANES), 1)
    packed = jnp.zeros((size, LANES), f32)
    for spot, piece in enumerate(split3(lse) + split3(delta)):
        packed = jnp.where(lane == spot, piece, packed)
    return vectors, packed


def attend_pieces(pieces, members, places, keys, lay):
    place, rows = lax.axis_index("seq"), lay.rows
    query = jnp.concatenate([piece[0:rows, :] for piece in pieces], axis=0)
    grad = jnp.concatenate([piece[rows:2 * rows, :] for piece in pieces], axis=0)
    limits = jnp.concatenate(
        [places[pl.ds(pl.multiple_of((place ^ m) * rows, 16), rows), :] for m in members], axis=0)
    return attend(query, grad, limits, [ref[...] for ref in keys], place, lay.scale)


def early_kernel(*refs, lay):
    members = lay.early
    pieces, refs = refs[:len(members)], refs[len(members):]
    places, keys, own, sent, packed = refs[0], refs[1:5], refs[5], refs[6:-1], refs[-1]
    vectors, packed[...] = attend_pieces(pieces, members, places, keys, lay)
    rows = lay.rows
    for which in range(3):
        span = slice(which * rows, (which + 1) * rows)
        own[span, :] = vectors[which][0:rows]
        for n, target in enumerate(sent):
            target[span, :] = vectors[which][(n + 1) * rows:(n + 2) * rows].astype(bf16)


def stat_rows_of(columns, coded, tiles):
    stats = [columns[k * LANES:(k + 1) * LANES, :].T[0:8, :] for k in range(tiles)]
    for k in range(tiles):
        coded[:, k * LANES:(k + 1) * LANES] = stats[k]
    return jnp.concatenate(stats, axis=0).astype(bf16)


def late_kernel(*refs, lay):
    early, late, rows = lay.early, lay.late, lay.rows
    pieces, refs = refs[:len(late)], refs[len(late):]
    places, keys, packed, refs = refs[0], refs[1:5], refs[5], refs[6:]
    sent, refs = refs[:len(early) - 1], refs[len(early) - 1:]
    coded, messages, columns = refs[0], refs[1:-1], refs[-1]
    place = lax.axis_index("seq")
    vectors, stats = attend_pieces(pieces, late, places, keys, lay)
    columns[...] = jnp.zeros(columns.shape, f32)
    for source, members in ((packed[...], early), (stats, late)):
        for n, m in enumerate(members):
            start = pl.multiple_of((place ^ m) * rows, 16)
            columns[pl.ds(start, rows), :] = source[n * rows:(n + 1) * rows]
    stat_rows = stat_rows_of(columns, coded, lay.tiles)
    for m, message in enumerate(messages, 1):
        if m in late:
            n = late.index(m)
            for which in range(3):
                message[which * rows:(which + 1) * rows, :] = (
                    vectors[which][n * rows:(n + 1) * rows].astype(bf16))
        else:
            message[0:3 * rows, :] = sent[early.index(m) - 1][...]
        message[3 * rows:, :] = stat_rows


def forward_kernel(gathered, root_k, root_v, branch_k, branch_v, places,
                   own, coded, messages, vectors, query_rows, grad_rows, *, lay):
    place = lax.axis_index("seq")
    rows, total, tiles = lay.rows, lay.total, lay.tiles
    arrange(place, gathered, 0, query_rows, grad_rows, 0, lay)
    keys = root_k[...], root_v[...], branch_k[...], branch_v[...]
    stat_columns = []
    for at, size in cut(total, 384):
        span = slice(at, at + size)
        parts, packed = attend(query_rows[span, :], grad_rows[span, :], places[span, :], keys, place, lay.scale)
        for which in range(3):
            vectors[which, span, :] = parts[which]
        stat_columns.append(packed)
    if tiles * LANES > total:
        stat_columns.append(jnp.zeros((tiles * LANES - total, LANES), f32))
    stat_rows = stat_rows_of(jnp.concatenate(stat_columns, axis=0), coded, tiles)

    def piece(which, target):
        return vectors[which, pl.ds(pl.multiple_of(target * rows, 16), rows), :]

    for which in range(3):
        span = slice(which * rows, (which + 1) * rows)
        own[span, :] = piece(which, place)
        for target in range(lay.count):
            messages[target, span, :] = piece(which, target).astype(bf16)
    for target in range(lay.count):
        messages[target, 3 * rows:, :] = stat_rows


def combine_kernel(coded, *rest, lay):
    messages, final, every = rest[:-2], rest[-2], rest[-1]
    rows, count = lay.rows, lay.count
    final[...] = jnp.zeros(final.shape, f32)
    every[...] = jnp.zeros(every.shape, f32)
    for k in range(lay.tiles):
        span = slice(k * LANES, (k + 1) * LANES)
        stats = [coded[:, span]]
        for message in messages:
            both = message[3 * rows + 16 * (k // 2):3 * rows + 16 * (k // 2) + 16, :].astype(f32)
            stats.append(both[8 * (k % 2):8 * (k % 2) + 8, :])
        lses = [s[0:1] + s[1:2] + s[2:3] for s in stats]
        deltas = [s[3:4] + s[4:5] + s[5:6] for s in stats]
        peak = functools.reduce(jnp.maximum, lses)
        shares = [jnp.exp2(v - peak) for v in lses]
        norm = total_of(shares)
        final[0:1, span] = peak + jnp.log(norm) * LOG2E
        final[1:2, span] = total_of([a * b for a, b in zip(shares, deltas)]) / norm
        for v in range(count):
            every[v:v + 1, span] = lses[v]
            every[count + v:count + v + 1, span] = deltas[v]


def local_weights(parts, query, grad, probs, slopes, local, line, logits, products, scale):
    block = 256
    for row, width in cut(query.shape[0], 384):
        lanes = slice(row, row + width)
        q, g = query[lanes, :], grad[lanes, :]
        peak = jnp.full((1, width), NEG, f32)
        spots = []
        for start, keys, values, visible in parts:
            for at in range(0, keys.shape[0], block):
                size = min(block, keys.shape[0] - at)
                s = nt(keys[at:at + size, :], q) * (scale * LOG2E)
                if visible is not None:
                    s = jnp.where(visible(at, size, lanes), s, NEG)
                logits[start + at:start + at + size, 0:width] = s
                products[start + at:start + at + size, 0:width] = nt(values[at:at + size, :], g)
                peak = jnp.maximum(peak, jnp.max(s, axis=0, keepdims=True))
                spots.append(slice(start + at, start + at + size))
        norm = jnp.zeros((1, width), f32)
        weighted = jnp.zeros((1, width), f32)
        for spot in spots:
            p = jnp.exp2(logits[spot, 0:width] - peak)
            logits[spot, 0:width] = p
            probs[spot, lanes] = p.astype(bf16)
            norm = norm + jnp.sum(p, axis=0, keepdims=True)
            weighted = weighted + jnp.sum(p * products[spot, 0:width], axis=0, keepdims=True)
        delta = weighted / norm
        for spot in spots:
            slopes[spot, lanes] = (logits[spot, 0:width] * (products[spot, 0:width] - delta)).astype(bf16)
        local[line:line + 1, lanes] = peak
        local[line + 1:line + 2, lanes] = delta


def own_pre_kernel(mine, other, places, root_k, root_v, branch_k, branch_v,
                   probs, slopes, local, query, grad, logits, products, *, lay):
    place, half = lax.axis_index("seq"), lax.axis_index("head")
    arrange(place, mine, 0, query, grad, half * lay.total, lay)
    arrange(place, other, 0, query, grad, (1 - half) * lay.total, lay)
    count = branch_k.shape[0]

    def visible(at, size, lanes):
        spot = (place * count + at) + lax.broadcasted_iota(jnp.int32, (size, lanes.stop - lanes.start), 0)
        return spot <= places[0:1, lanes]

    local_weights([(0, branch_k, branch_v, visible)], query, grad, probs, slopes, local, 0,
                  logits, products, lay.scale)
    local_weights([(count, root_k, root_v, None)], query, grad, probs, slopes, local, 2,
                  logits, products, lay.scale)


def other_pre_kernel(pair, root_k, root_v, probs, slopes, local, query, grad,
                     logits, products, *, lay):
    place, half = lax.axis_index("seq"), lax.axis_index("head") ^ FAR_FLIP
    arrange(place, pair, 0, query, grad, half * lay.total, lay)
    arrange(place, pair, 2 * lay.total, query, grad, (1 - half) * lay.total, lay)
    local_weights([(0, root_k, root_v, None)], query, grad, probs, slopes, local, 2,
                  logits, products, lay.scale)


def scaled_rows(local, line, stats, query, grad, both, single, scale):
    for k in range(query.shape[0] // LANES):
        span = slice(k * LANES, (k + 1) * LANES)
        weight = jnp.exp2(local[line:line + 1, span] - stats[0:1, span])
        shift = weight * (local[line + 1:line + 2, span] - stats[1:2, span])
        stacked = jnp.concatenate([weight, shift, jnp.zeros((LANES - 2, LANES), f32)], axis=0)
        columns = stacked.T
        weight, shift = columns[:, 0:1], columns[:, 1:2]
        q = query[span, :].astype(f32) * scale
        both[span, 0:LANES] = (grad[span, :].astype(f32) * weight).astype(bf16)
        both[span, LANES:] = (q * shift).astype(bf16)
        single[span, :] = (q * weight).astype(bf16)


def gradients(probs, slopes, spot, both, single):
    wide = nn(probs[spot, :], both[...])
    return wide[:, LANES:] + nn(slopes[spot, :], single[...]), wide[:, 0:LANES]


def finish_kernel(own, every, *rest, lay):
    messages, (out_a, out_q, columns) = rest[:-3], rest[-3:]
    rows, count = lay.rows, lay.count
    tall = every.shape[0]
    for k in range(lay.tiles):
        piece = every[:, k * LANES:(k + 1) * LANES]
        if tall < LANES:
            piece = jnp.concatenate([piece, jnp.zeros((LANES - tall, LANES), f32)], axis=0)
        columns[k * LANES:(k + 1) * LANES, :] = piece.T
    mine_rows = columns[pl.ds(pl.multiple_of(lax.axis_index("seq") * rows, 16), rows), :]
    lses = [mine_rows[:, v:v + 1] for v in range(count)]
    deltas = [mine_rows[:, count + v:count + v + 1] for v in range(count)]
    peak = functools.reduce(jnp.maximum, lses)
    shares = [jnp.exp2(v - peak) for v in lses]
    inverse = 1.0 / total_of(shares)
    shares = [s * inverse for s in shares]
    delta = total_of([a * b for a, b in zip(shares, deltas)])
    attended = jnp.zeros((rows, LANES), f32)
    slope_sum = jnp.zeros((rows, LANES), f32)
    for v in range(count):
        source = own if v == 0 else messages[v - 1]
        o_part = source[0:rows, :].astype(f32)
        a_part = source[rows:2 * rows, :].astype(f32)
        b_part = source[2 * rows:3 * rows, :].astype(f32)
        attended = attended + shares[v] * o_part
        slope_sum = slope_sum + shares[v] * (a_part + (deltas[v] - delta) * b_part)
    out_a[...] = attended.reshape(out_a.shape).astype(bf16)
    out_q[...] = (slope_sum * lay.scale).reshape(out_q.shape)


def own_final_kernel(probs, slopes, local, query, grad, stats,
                     acc_k, acc_v, branch_k, branch_v, both, single, *, lay):
    count = branch_k.shape[0]
    block = 512
    for base, line, to_k, to_v in ((0, 0, branch_k, branch_v), (count, 2, acc_k, acc_v)):
        scaled_rows(local, line, stats, query, grad, both, single, lay.scale)
        for at in range(0, to_k.shape[0], block):
            size = min(block, to_k.shape[0] - at)
            to_k[at:at + size, :], to_v[at:at + size, :] = gradients(
                probs, slopes, slice(base + at, base + at + size), both, single)


def other_final_kernel(probs, slopes, local, query, grad, stats, acc_k, acc_v,
                       branch_k, branch_v, attended, query_grad,
                       out_k, out_v, out_bk, out_bv, out_a, out_q,
                       both, single, hold_k, hold_v, sems, *, lay):
    copies = []

    def send(source, target, sem):
        copies.append(pltpu.make_async_copy(source, target, sem))
        copies[-1].start()

    send(branch_k, out_bk, sems.at[2, 0])
    send(branch_v, out_bv, sems.at[2, 1])
    send(attended, out_a, sems.at[3, 0])
    send(query_grad, out_q, sems.at[3, 1])
    scaled_rows(local, 2, stats, query, grad, both, single, lay.scale)
    count = hold_k.shape[0]
    block = 256
    for n, at in enumerate(range(0, count, block)):
        spot = slice(at, min(at + block, count))
        more_k, more_v = gradients(probs, slopes, spot, both, single)
        hold_k[spot, :] = acc_k[spot, :] + more_k
        send(hold_k.at[spot, :], out_k.at[spot, :], sems.at[0, n])
        hold_v[spot, :] = acc_v[spot, :] + more_v
        send(hold_v.at[spot, :], out_v.at[spot, :], sems.at[1, n])
    for copy in copies:
        copy.wait()


class Lay:
    def __init__(self, count, rows, scale):
        self.count, self.rows, self.scale = count, rows, scale
        self.total = count * rows
        self.tiles = lane_tiles(self.total)
        self.bits = list(range(count.bit_length() - 1))
        self.swap = 1 < count <= 4
        self.early = [m for m in (0, 2) if m < count]
        self.late = [m for m in range(1, count) if m not in self.early]


VMEM = pl.BlockSpec(memory_space=pltpu.VMEM)
ANY = pl.BlockSpec(memory_space=pl.ANY)
HBM = pl.BlockSpec(memory_space=pltpu.HBM)


def call(kernel, lay, args, outs, scratch=(), away=0, far=False):
    specs = [VMEM] * (len(outs) - away) + [ANY] * away
    limit = (20 if lay.total <= 384 else 50) * 2**20
    if far:
        args = [pltpu.with_memory_space_constraint(value, pltpu.HBM) for value in args]
    return pl.pallas_call(
        functools.partial(kernel, lay=lay),
        out_shape=[jax.ShapeDtypeStruct(shape, kind) for shape, kind in outs],
        in_specs=[HBM if far else VMEM] * len(args), out_specs=specs, scratch_shapes=list(scratch),
        compiler_params=pltpu.CompilerParams(vmem_limit_bytes=limit),
    )(*args)


def per_device(mesh, queries, output_cotangent, root_keys, root_values,
               branch_keys, branch_values, answer_positions):
    return body(mesh, queries, output_cotangent, root_keys, root_values,
                branch_keys, branch_values, answer_positions)


def body(mesh, queries, output_cotangent, root_keys, root_values,
         branch_keys, branch_values, answer_positions):
    count, branches, heads = mesh.shape["seq"], mesh.shape["branch"], mesh.shape["head"]
    _, answers_here, heads_here, width = queries.shape
    rows = answers_here * heads_here
    lay = Lay(count, rows, 1.0 / math.sqrt(width))
    total, tiles = lay.total, lay.tiles
    lanes = heads * total
    root_count = root_keys.shape[0]
    branch_count = branch_keys.shape[1]
    seq_index = lax.axis_index("seq")
    head_index = lax.axis_index("head")
    crossing = lay.swap and heads == 2

    def seq_pairs(m):
        flip = SEQ_FLIPS[m] if crossing else 0
        return [(z * heads + c, (z ^ m) * heads + (c ^ flip)) for z in range(count) for c in range(heads)]

    def far_pairs(m, flip):
        return [(b * heads + c, (b + m) % branches * heads + (c ^ flip))
                for b in range(branches) for c in range(heads)]

    swap_heads = [(i, (i + 1) % heads) for i in range(heads)]
    shifts = range(1, branches)

    gathered = jnp.concatenate([queries.reshape(rows, width), output_cotangent.reshape(rows, width)], 0)
    gathered = lax.optimization_barrier(gathered)
    packed = gathered
    if lay.swap:
        arrived = [packed] + [lax.ppermute(packed, ("seq", "head"), seq_pairs(m)) for m in range(1, count)]
        gathered = jnp.concatenate(arrived, 0)
    else:
        for bit in lay.bits:
            pairs = seq_pairs(1 << bit)
            gathered = jnp.concatenate([gathered, lax.ppermute(gathered, ("seq", "head"), pairs)], 0)
    key_shapes = [((root_count, width), bf16)] * 2 + [((branch_count, width), bf16)] * 2
    root_k, root_v, branch_k, branch_v, place_column, place_row = call(
        prepare_kernel, lay, (root_keys, root_values, branch_keys[0], branch_values[0], answer_positions),
        key_shapes + [((lanes, 1), jnp.int32), ((8, lanes), jnp.int32)],
        [pltpu.VMEM(answer_positions.shape, jnp.int32), pltpu.SemaphoreType.DMA((5,))], far=True)
    other = lax.ppermute(gathered, "head", swap_heads)

    message_rows = 3 * rows + 8 * tiles
    keys = (root_k, root_v, branch_k, branch_v)
    stat_shape, own_shape = ((8, tiles * LANES), f32), ((3 * rows, width), f32)
    if lay.swap:
        own, *sent, packed_stats = call(
            early_kernel, lay, (*[arrived[m] for m in lay.early], place_column, *keys),
            [own_shape] + [((3 * rows, width), bf16)] * (len(lay.early) - 1)
            + [((len(lay.early) * rows, LANES), f32)])
        coded, *messages = call(
            late_kernel, lay,
            (*[arrived[m] for m in lay.late], place_column, *keys, packed_stats, *sent),
            [stat_shape] + [((message_rows, width), bf16)] * (count - 1),
            [pltpu.VMEM((tiles * LANES, LANES), f32)])
        received = [lax.ppermute(message, ("seq", "head"), seq_pairs(m + 1))
                    for m, message in enumerate(messages)]
    else:
        own, coded, messages = call(
            forward_kernel, lay, (gathered, *keys, place_column),
            [own_shape, stat_shape, ((count, message_rows, width), bf16)],
            [pltpu.VMEM((3, total, width), f32), pltpu.VMEM((total, width), bf16),
             pltpu.VMEM((total, width), bf16)])
        whole = lax.all_to_all(messages, "seq", split_axis=0, concat_axis=0, tiled=True)
        received = [lax.dynamic_index_in_dim(whole, seq_index ^ m, 0, keepdims=False)
                    for m in range(1, count)]

    pair = jnp.concatenate([gathered, other], 0)
    far = [lax.ppermute(pair, ("branch", "head"), far_pairs(m, FAR_FLIP if heads == 2 else 0)) for m in shifts]

    def weights_shapes(keys):
        shapes = [((keys, lanes), bf16), ((keys, lanes), bf16), ((8, lanes), f32),
                  ((lanes, width), bf16), ((lanes, width), bf16)]
        wide = cut(lanes, 384)[0][1]
        return shapes, [pltpu.VMEM((keys, wide), f32), pltpu.VMEM((keys, wide), f32)]

    shapes, scratch = weights_shapes(branch_count + root_count)
    own_pre = call(own_pre_kernel, lay,
                   (gathered, other, place_row, root_k, root_v, branch_k, branch_v),
                   shapes, scratch)

    tall = -(-2 * count // 8) * 8
    final, every = call(combine_kernel, lay, (coded, *received),
                        [((8, tiles * LANES), f32), ((tall, tiles * LANES), f32)])
    other_final = lax.ppermute(final, "head", swap_heads)
    a, b = final[:, :total], other_final[:, :total]
    stats = jnp.where(head_index == 0, jnp.concatenate([a, b], 1), jnp.concatenate([b, a], 1))
    far_stats = [lax.ppermute(stats, ("branch", "head"), far_pairs(m, STAT_FLIP if heads == 2 else 0)) for m in shifts]

    def final_scratch(keys):
        blocks = -(-keys // 256)
        return ([pltpu.VMEM((lanes, 2 * width), bf16), pltpu.VMEM((lanes, width), bf16)],
                [pltpu.VMEM((keys, width), f32), pltpu.VMEM((keys, width), f32),
                 pltpu.SemaphoreType.DMA((4, max(2, blocks)))])

    row_shapes = [((answers_here, heads_here, width), bf16), ((answers_here, heads_here, width), f32)]
    attention, query_grad = call(
        finish_kernel, lay, (own, every, *received),
        row_shapes, [pltpu.VMEM((tiles * LANES, LANES), f32)])
    root_sum, branch_sum = ((root_count, width), f32), ((branch_count, width), f32)
    first, last = final_scratch(root_count)
    acc_k, acc_v, branch_gk, branch_gv = call(
        own_final_kernel, lay, (*own_pre, stats),
        [root_sum, root_sum, branch_sum, branch_sum], first)
    shapes, scratch = weights_shapes(root_count)
    for pair, pair_stats in zip(far, far_stats):
        pre = call(other_pre_kernel, lay, (pair, root_k, root_v),
                   shapes, scratch)
        acc_k, acc_v, branch_gk, branch_gv, attention, query_grad = call(
            other_final_kernel, lay,
            (*pre, pair_stats, acc_k, acc_v, branch_gk, branch_gv, attention, query_grad),
            [root_sum, root_sum, branch_sum, branch_sum, *row_shapes], first + last, away=6)
    return (attention[None], query_grad[None], acc_k, acc_v, branch_gk[None], branch_gv[None])


def solution(mesh):
    rows = P(("parts", "branch"), "seq", "head", None)
    root = P(("parts", "seq"), None)
    branch = P(("parts", "branch"), "seq", None)
    return jax.shard_map(
        functools.partial(per_device, mesh),
        mesh=mesh,
        in_specs=(rows, rows, root, root, branch, branch, P(("parts", "branch"), None)),
        out_specs=(rows, rows, root, root, branch, branch),
        check_vma=False,
    )
```
